128 devices in a mesh: rep: 64 (over z, y, x), data: 2 (over core).
Axes of the slice: x: 4, y: 4, z: 4, core: 2. Of those that a mesh axis runs over, the one named last changes fastest.
Arguments:
- act_in: bfloat16 [131072, 1024], P(('rep', 'data'))
- grad_out: bfloat16 [131072, 1024], P(('rep', 'data'))
- w_one: bfloat16 [1024, 3072], replicated
- w_two: bfloat16 [3072, 1024], replicated
- w_three: bfloat16 [1024, 3072], replicated
- w_four: bfloat16 [3072, 1024], replicated
- master_one: float32 [1024, 3072], P('data')
- master_two: float32 [3072, 1024], P('data')
- master_three: float32 [1024, 3072], P('data')
- master_four: float32 [3072, 1024], P('data')
- mom_one: float32 [1024, 3072], P('data')
- mom_two: float32 [3072, 1024], P('data')
- mom_three: float32 [1024, 3072], P('data')
- mom_four: float32 [3072, 1024], P('data')
- vel_one: float32 [1024, 3072], P('data')
- vel_two: float32 [3072, 1024], P('data')
- vel_three: float32 [1024, 3072], P('data')
- vel_four: float32 [3072, 1024], P('data')
- clip_norm: float32 [], replicated
Outputs:
- output 1: bfloat16 [1024, 3072], replicated
- output 2: bfloat16 [3072, 1024], replicated
- output 3: bfloat16 [1024, 3072], replicated
- output 4: bfloat16 [3072, 1024], replicated
- output 5: float32 [1024, 3072], P('data')
- output 6: float32 [3072, 1024], P('data')
- output 7: float32 [1024, 3072], P('data')
- output 8: float32 [3072, 1024], P('data')
- output 9: float32 [1024, 3072], P('data')
- output 10: float32 [3072, 1024], P('data')
- output 11: float32 [1024, 3072], P('data')
- output 12: float32 [3072, 1024], P('data')
- output 13: float32 [1024, 3072], P('data')
- output 14: float32 [3072, 1024], P('data')
- output 15: float32 [1024, 3072], P('data')
- output 16: float32 [3072, 1024], P('data')
- output 17: float32 [], replicated
All inputs are finite; a program needn't handle non-finite values.
Results may differ from the reference program's by a relative error of at most 0.00368133.
Values are sent between devices in bfloat16 or wider.
A program may use at most 1 GiB of HBM per device.

```python
import jax
import jax.numpy as jnp
from jax import lax

D = 1024
FF = 3072
TOK_DEV = 1024
DEVICES = 128
TRAIN_STEP = 10
BATCH = TOK_DEV * DEVICES
BETA_ONE = 0.9
BETA_TWO = 0.95
ADAM_EPS = 1e-8
NORM_EPS = 1e-6
LEARN_RATE = 0.003


def gelu_fn(values):
    return jax.nn.gelu(values, approximate=True)


def local_grads(act_in, grad_out, w_one, w_two, w_three, w_four):
    h_one = jnp.dot(act_in, w_one, preferred_element_type=jnp.float32).astype(jnp.bfloat16)
    a_one_f, back_one = jax.vjp(gelu_fn, h_one.astype(jnp.float32))
    a_one = a_one_f.astype(jnp.bfloat16)
    y_one = jnp.dot(a_one, w_two, preferred_element_type=jnp.float32).astype(jnp.bfloat16)
    h_two = jnp.dot(y_one, w_three, preferred_element_type=jnp.float32).astype(jnp.bfloat16)
    a_two_f, back_two = jax.vjp(gelu_fn, h_two.astype(jnp.float32))
    a_two = a_two_f.astype(jnp.bfloat16)
    g_four = jnp.dot(a_two.T, grad_out, preferred_element_type=jnp.float32)
    da_two = jnp.dot(grad_out, w_four.T, preferred_element_type=jnp.float32).astype(jnp.bfloat16)
    dh_two = back_two(da_two.astype(jnp.float32))[0].astype(jnp.bfloat16)
    g_three = jnp.dot(y_one.T, dh_two, preferred_element_type=jnp.float32)
    dy_one = jnp.dot(dh_two, w_three.T, preferred_element_type=jnp.float32).astype(jnp.bfloat16)
    g_two = jnp.dot(a_one.T, dy_one, preferred_element_type=jnp.float32)
    da_one = jnp.dot(dy_one, w_two.T, preferred_element_type=jnp.float32).astype(jnp.bfloat16)
    dh_one = back_one(da_one.astype(jnp.float32))[0].astype(jnp.bfloat16)
    g_one = jnp.dot(act_in.T, dh_one, preferred_element_type=jnp.float32)
    return g_one, g_two, g_three, g_four


def total_grads(act_in, grad_out, w_one, w_two, w_three, w_four):
    act_blocks = act_in.reshape(DEVICES, TOK_DEV, D)
    out_blocks = grad_out.reshape(DEVICES, TOK_DEV, D)
    init_sums = (jnp.zeros((D, FF), jnp.float32), jnp.zeros((FF, D), jnp.float32), jnp.zeros((D, FF), jnp.float32), jnp.zeros((FF, D), jnp.float32))

    def scan_step(acc_sums, blocks):
        block_grads = local_grads(blocks[0], blocks[1], w_one, w_two, w_three, w_four)
        return tuple(acc_val + new_val for acc_val, new_val in zip(acc_sums, block_grads)), None

    summed, _ = lax.scan(scan_step, init_sums, (act_blocks, out_blocks))
    return tuple(sum_val / DEVICES for sum_val in summed)


def global_norm(grad_list):
    return jnp.sqrt(sum(jnp.sum(jnp.square(gradient)) for gradient in grad_list))


def adam_update(gradient, master, mom_in, vel_in, clip_scale):
    scaled = clip_scale * gradient
    mom_new = BETA_ONE * mom_in + (1.0 - BETA_ONE) * scaled
    vel_new = BETA_TWO * vel_in + (1.0 - BETA_TWO) * jnp.square(scaled)
    corr_one = 1.0 - BETA_ONE ** TRAIN_STEP
    corr_two = 1.0 - BETA_TWO ** TRAIN_STEP
    master_new = master - LEARN_RATE * (mom_new / corr_one) / (jnp.sqrt(vel_new / corr_two) + ADAM_EPS)
    return master_new, mom_new, vel_new


def setup_inputs(seed: int = 0) -> dict:
    key_list = jax.random.split(jax.random.key(seed), 16)
    act_in = jax.random.normal(key_list[0], (BATCH, D), jnp.float32).astype(jnp.bfloat16)
    grad_out = jax.random.normal(key_list[1], (BATCH, D), jnp.float32).astype(jnp.bfloat16)
    shape_list = ((D, FF), (FF, D), (D, FF), (FF, D))
    std_list = (D ** -0.5, 2.0 * FF ** -0.5, D ** -0.5, 2.0 * FF ** -0.5)
    master_list = [jax.random.normal(key_list[2 + mat_idx], shape_list[mat_idx], jnp.float32) * std_list[mat_idx] for mat_idx in range(4)]
    weight_list = [master.astype(jnp.bfloat16) for master in master_list]
    grad_list = total_grads(act_in, grad_out, weight_list[0], weight_list[1], weight_list[2], weight_list[3])
    grad_norm = global_norm(grad_list)
    clip_norm = grad_norm * jax.random.uniform(key_list[6], (), jnp.float32, minval=0.3, maxval=0.7)
    clip_scale = clip_norm / grad_norm
    rms_list = [clip_scale * jnp.sqrt(jnp.mean(jnp.square(gradient))) for gradient in grad_list]
    mom_list = [0.4 * rms_list[mat_idx] * jax.random.normal(key_list[7 + mat_idx], shape_list[mat_idx], jnp.float32) for mat_idx in range(4)]
    vel_list = [jnp.square(rms_list[mat_idx]) * jax.random.uniform(key_list[11 + mat_idx], shape_list[mat_idx], jnp.float32, minval=0.1, maxval=1.0) for mat_idx in range(4)]
    return {'act_in': act_in, 'grad_out': grad_out, 'w_one': weight_list[0], 'w_two': weight_list[1], 'w_three': weight_list[2], 'w_four': weight_list[3], 'master_one': master_list[0], 'master_two': master_list[1], 'master_three': master_list[2], 'master_four': master_list[3], 'mom_one': mom_list[0], 'mom_two': mom_list[1], 'mom_three': mom_list[2], 'mom_four': mom_list[3], 'vel_one': vel_list[0], 'vel_two': vel_list[1], 'vel_three': vel_list[2], 'vel_four': vel_list[3], 'clip_norm': clip_norm}


def reference(act_in, grad_out, w_one, w_two, w_three, w_four, master_one, master_two, master_three, master_four, mom_one, mom_two, mom_three, mom_four, vel_one, vel_two, vel_three, vel_four, clip_norm):
    grad_list = total_grads(act_in, grad_out, w_one, w_two, w_three, w_four)
    grad_norm = global_norm(grad_list)
    clip_scale = jnp.minimum(1.0, clip_norm / (grad_norm + NORM_EPS))
    upd_one = adam_update(grad_list[0], master_one, mom_one, vel_one, clip_scale)
    upd_two = adam_update(grad_list[1], master_two, mom_two, vel_two, clip_scale)
    upd_three = adam_update(grad_list[2], master_three, mom_three, vel_three, clip_scale)
    upd_four = adam_update(grad_list[3], master_four, mom_four, vel_four, clip_scale)
    return (upd_one[0].astype(jnp.bfloat16), upd_two[0].astype(jnp.bfloat16), upd_three[0].astype(jnp.bfloat16), upd_four[0].astype(jnp.bfloat16), upd_one[0], upd_two[0], upd_three[0], upd_four[0], upd_one[1], upd_two[1], upd_three[1], upd_four[1], upd_one[2], upd_two[2], upd_three[2], upd_four[2], grad_norm)
```

```python
import jax
import jax.numpy as jnp
from jax import lax
from jax.experimental import pallas as pl
from jax.experimental.pallas import tpu as pltpu
from jax.sharding import PartitionSpec as P

TRAIN_STEP = 10
BETA_ONE = 0.9
BETA_TWO = 0.95
ADAM_EPS = 1e-8
NORM_EPS = 1e-6
LEARN_RATE = 0.003
STEP_SIZE = LEARN_RATE / (1.0 - BETA_ONE ** TRAIN_STEP)
VEL_GAIN = 1.0 / (1.0 - BETA_TWO ** TRAIN_STEP)
MESH = pl.DeviceIdType.MESH
NMAT = 4
F32 = jnp.float32
D = 1024
FF = 3072
HALF = 512
TILE = 256
HALF_SHAPE = ((64, 1024), (16, 1024), (8, 512))
CHUNK_ROWS = (128, 32, 8)
AXES = 3
RING = 4
BOTH = 2
NSET = 2


class Torus:
    def __init__(self):
        self.rep = lax.axis_index('rep')
        self.core = lax.axis_index('data')

    def stride(self, axis):
        return 1 + 3 * lax.rem(axis, 3) + 9 * lax.div(lax.rem(axis, 3), 2)

    def pos(self, axis):
        return lax.rem(lax.div(self.rep, self.stride(axis)), 4)

    def peer(self, axis, delta):
        stride = self.stride(axis)
        pos = lax.rem(lax.div(self.rep, stride), 4)
        return {'rep': self.rep + (lax.rem(pos + delta + 4, 4) - pos) * stride, 'data': self.core}


class Exchange:
    def __init__(self, tor, grads, slots, norm_buf, rs_send, rs_recv, ag_send, ag_recv, free_sem, slot_sem, nm_send, nm_recv):
        self.free_sem, self.slot_sem = free_sem, slot_sem
        self.tor, self.grads, self.slots = tor, grads, slots
        self.pos = [tor.pos(axis) for axis in range(AXES)]
        self.base = []
        for stream in range(AXES):
            base = stream * HALF
            for level in range(AXES):
                self.base.append(base)
                base = base + self.pos[(stream + level) % AXES] * CHUNK_ROWS[level]
        self.norm_buf = norm_buf
        self.rs_send, self.rs_recv, self.ag_send, self.ag_recv = rs_send, rs_recv, ag_send, ag_recv
        self.nm_send, self.nm_recv = nm_send, nm_recv

    def neighbour(self, stream, level, side):
        axis = (stream + level) % AXES
        pos = self.pos[axis]
        return {'rep': self.tor.rep + (lax.rem(pos + 1 + BOTH * side, RING) - pos) * RING ** axis, 'data': self.tor.core}

    def region(self, mat, stream, level, delta, half):
        rows = CHUNK_ROWS[level]
        row = self.base[stream * AXES + level] + lax.rem(self.pos[(stream + level) % AXES] + delta, RING) * rows
        if level < BOTH:
            row = pl.multiple_of(row + half * (rows // BOTH), rows // BOTH)
            return self.grads.at[mat, pl.ds(row, rows // BOTH), :]
        return self.grads.at[mat, pl.ds(pl.multiple_of(row, rows), rows), pl.ds(pl.multiple_of(half * HALF, HALF), HALF)]

    def rs_copy(self, mat, stream, level, msg, side):
        near = 1 + BOTH * side
        if isinstance(msg, int):
            delta, half = ((BOTH, side), (near, 1 - side), (near, side))[msg]
        else:
            delta, half = BOTH + msg * (near - BOTH), side + msg * (1 - BOTH * side)
        return pltpu.make_async_remote_copy(
            src_ref=self.region(mat, stream, level, delta, half),
            dst_ref=self.slots[level].at[lax.rem(mat, NSET), stream, msg, side],
            send_sem=self.rs_send.at[mat, level],
            recv_sem=self.rs_recv.at[mat, level, msg - msg // BOTH if isinstance(msg, int) else msg],
            device_id=self.neighbour(stream, level, side), device_id_type=MESH)

    def ag_copy(self, mat, stream, level, msg, side):
        if isinstance(msg, int):
            delta, half = ((0, side), (0, 1 - side), (RING - 1 - BOTH * side, side))[msg]
        else:
            delta, half = 0, side + msg * (1 - BOTH * side)
        ref = self.region(mat, stream, level, delta, half)
        return pltpu.make_async_remote_copy(
            src_ref=ref, dst_ref=ref,
            send_sem=self.ag_send.at[mat, level],
            recv_sem=self.ag_recv.at[mat, level, msg - msg // BOTH if isinstance(msg, int) else msg],
            device_id=self.neighbour(stream, level, side), device_id_type=MESH)

    def pairs(self, body, msgs=1):
        for stream in range(AXES):
            def one(idx, carry, stream=stream):
                body(stream, lax.rem(idx, BOTH), lax.div(idx, BOTH))
                return carry
            lax.fori_loop(0, BOTH * msgs, one, 0)

    def bulk(self, mat, level, late, gather):
        send, recv = (self.ag_send, self.ag_recv) if gather else (self.rs_send, self.rs_recv)
        count = AXES * BOTH * (AXES if late is None else 1 + late)
        rows = count * HALF_SHAPE[level][0] * HALF_SHAPE[level][1] // D
        ref = self.grads.at[mat, pl.ds(0, rows), :]
        copy = pltpu.make_async_remote_copy(src_ref=ref, dst_ref=ref, send_sem=send.at[mat, level], recv_sem=recv.at[mat, level, late or 0], device_id=self.neighbour(0, level, 0), device_id_type=MESH)
        if late is None:
            copy.wait_send()
        else:
            copy.wait_recv()

    def rs_first(self, mat, level):
        @pl.when(mat < NMAT - NSET)
        def _():
            pl.semaphore_wait(self.slot_sem.at[mat, level], AXES * BOTH)
        self.pairs(lambda stream, side, msg: self.rs_copy(mat, stream, level, msg, side).start(), BOTH)

    def rs_mid(self, mat, level):
        self.bulk(mat, level, 0, False)

        def body(stream, side, _):
            ref = self.region(mat, stream, level, 1 + BOTH * side, side)
            ref[...] = ref[...] + self.slots[level][lax.rem(mat, NSET), stream, 0, side]
            self.rs_copy(mat, stream, level, BOTH, side).start()
        self.pairs(body)

    def rs_last(self, mat, level):
        self.bulk(mat, level, 1, False)
        self.bulk(mat, level, None, False)

        def body(stream, half, _):
            ref = self.region(mat, stream, level, 0, half)
            held = self.slots[level]
            total = ref[...] + held[lax.rem(mat, NSET), stream, 2, half] + held[lax.rem(mat, NSET), stream, 1, 1 - half]
            if level == 2:
                total = total * (1.0 / 128.0)
                square = total * total
                self.norm_buf[4, 0] = self.norm_buf[4, 0] + sum(square[:, col * 128:(col + 1) * 128] for col in range(RING))
            ref[...] = total
        self.pairs(body)

        def tell(stream, side, _):
            peer = self.neighbour(stream, level, side)
            pl.semaphore_signal(self.free_sem.at[mat, level], inc=1, device_id=peer, device_id_type=MESH)

            @pl.when(mat >= NSET)
            def _():
                pl.semaphore_signal(self.slot_sem.at[mat - NSET, level], inc=1, device_id=peer, device_id_type=MESH)
        self.pairs(tell)

    def ag_first(self, mat, level):
        pl.semaphore_wait(self.free_sem.at[mat, level], AXES * BOTH)
        self.pairs(lambda stream, side, msg: self.ag_copy(mat, stream, level, msg, side).start(), BOTH)

    def ag_mid(self, mat, level):
        self.bulk(mat, level, 0, True)
        self.pairs(lambda stream, side, _: self.ag_copy(mat, stream, level, BOTH, side).start())

    def ag_last(self, mat, level):
        self.bulk(mat, level, 1, True)

    def step(self, mat, num):
        if num == 0:
            self.rs_first(mat, 0)
        elif num in (1, 3, 5):
            self.rs_mid(mat, num // 2)
        elif num in (2, 4):
            self.rs_last(mat, num // 2 - 1)
            self.rs_first(mat, num // 2)
        elif num == 6:
            self.rs_last(mat, 2)
            self.ag_first(mat, 2)
        elif num in (7, 9, 11):
            self.ag_mid(mat, 2 - (num - 7) // 2)
        elif num in (8, 10):
            level = 2 - (num - 8) // 2
            self.ag_last(mat, level)
            self.ag_first(mat, level - 1)
        else:
            self.ag_last(mat, 0)

    def norm_copy(self, stage, delta):
        tor = self.tor
        if stage < 3:
            mine, dev = tor.pos(stage), tor.peer(stage, delta)
        else:
            mine, dev = tor.core, {'data': 1 - tor.core}
        return pltpu.make_async_remote_copy(
            src_ref=self.norm_buf.at[4, stage], dst_ref=self.norm_buf.at[stage, mine],
            send_sem=self.nm_send.at[stage, delta], recv_sem=self.nm_recv.at[stage, delta],
            device_id=dev, device_id_type=MESH)

    def deltas(self, stage):
        return (1, 2, 3) if stage < AXES else (1,)

    def norm_start(self, stage):
        for delta in (self.deltas(stage)):
            self.norm_copy(stage, delta).start()
        mine = self.tor.pos(stage) if stage < 3 else self.tor.core
        self.norm_buf[stage, mine] = self.norm_buf[4, stage]

    def norm_finish(self, stage):
        for delta in (self.deltas(stage)):
            self.norm_copy(stage, delta).wait_recv()
        total = self.norm_buf[stage, 0] + self.norm_buf[stage, 1]
        if stage < 3:
            total = total + self.norm_buf[stage, 2] + self.norm_buf[stage, 3]
            self.norm_buf[4, stage + 1] = total
        else:
            self.norm_buf[4, 4] = total

    def drain(self):
        def one(mat, carry):
            for level in range(AXES):
                self.bulk(mat, level, None, True)
            return carry
        lax.fori_loop(0, NMAT, one, 0)
        for stage in range(4):
            for delta in (self.deltas(stage)):
                self.norm_copy(stage, delta).wait_send()

    def greet(self):
        tor = self.tor
        barrier = pltpu.get_barrier_semaphore()
        for axis in range(AXES):
            for delta in (1, 2, 3):
                pl.semaphore_signal(barrier, inc=1, device_id=tor.peer(axis, delta), device_id_type=MESH)
        pl.semaphore_signal(barrier, inc=1, device_id={'data': 1 - tor.core}, device_id_type=MESH)
        pl.semaphore_wait(barrier, 10)


SUB = 64
OCT = 8
LANE = 128
OWN = 1536
TILES = 6
HBM_ANY = pl.BlockSpec(memory_space=pl.ANY)
ROWS_ROWS = (((0,), (0,)), ((), ()))
COLS_COLS = (((1,), (1,)), ((), ()))
COMPUTE_SLOTS = 40
STEP_SLOTS = (
    (7, 11, 15, 17, 18, 22, 24, 25, 26, 31, 33, 46, 50),
    (17, 20, 24, 28, 40, 41, 43, 44, 45, 47, 50, 58, 64),
    (27, 31, 41, 42, 43, 44, 45, 46, 49, 55, 62, 72, 79),
    (39, 40, 41, 42, 43, 44, 45, 47, 60, 66, 76, 85, 92),
)
NORM_SLOTS = (45, 46, 47, 48, 50)
ADAM_RUNS = ((50, 48, 0),)
ADAM_READY = 42
LANES = 12
AHEAD = 8
PER_SLOT = 2
PIECES = 24
SLOTS = 98
GELU_A = 0.7978845608028654
GELU_B = 0.044715


def gelu_slope(hidden):
    square = hidden * hidden
    tanh = jnp.tanh(hidden * (GELU_A + GELU_A * GELU_B * square))
    return 0.5 * (1.0 + tanh) + (0.5 * hidden) * (1.0 - tanh * tanh) * (GELU_A + 3.0 * GELU_A * GELU_B * square)


N_ACTS = 11
N_STATE = 3


def take(refs, count, start=0):
    return refs[start:start + count]


def backward_kernel(*refs):
    x_in, dy_in, w_two, w_three, w_four, h_one, a_one, y_one, h_two, a_two, clip_ref = take(refs, N_ACTS)
    masters, moms, vels = (take(refs, NMAT, N_ACTS + which * NMAT) for which in range(N_STATE))
    outs = refs[N_ACTS + N_STATE * NMAT:]
    new_w, new_masters, new_moms, new_vels = (take(outs, NMAT, which * NMAT) for which in range(NMAT))
    norm_ref, x_peer, a_one_peer, a_two_peer = take(outs, NMAT, NMAT * NMAT)
    (grads, slot_big, slot_mid, slot_low, norm_buf, scale_ref, dh_own, dh_peer, dy_pair, y_pair, a_tile, w_tile, h_tile,
     rs_send, rs_recv, ag_send, ag_recv, free_sem, slot_sem, nm_send, nm_recv,
     a_tile_sem, w_tile_sem, h_tile_sem, load_sem, dyx_sem, yx_sem, xx_sem, a_one_sem, a_two_sem, dh_sem, dyp_sem,
     in_sem, out_sem, w_send, w_recv) = outs[NMAT * NMAT + NMAT:]
    tor = Torus()
    ex = Exchange(tor, grads, (slot_big, slot_mid, slot_low), norm_buf, rs_send, rs_recv, ag_send, ag_recv, free_sem, slot_sem, nm_send, nm_recv)
    core = tor.core
    other = 1 - core
    mate = {'data': other}

    def send(src, dst, sem):
        return pltpu.make_async_remote_copy(src_ref=src, dst_ref=dst, send_sem=sem.at[0], recv_sem=sem.at[1], device_id=mate, device_id_type=MESH)

    def columns(start, size):
        return pl.ds(pl.multiple_of(start, size), size)

    def piece_rows(index, base=0):
        return pl.ds(pl.multiple_of(base + index * SUB, SUB), SUB)

    dy_swap = send(dy_in, dy_pair.at[pl.ds(D, D), :], dyx_sem)
    y_swap = send(y_one.at[:, columns(other * HALF, HALF)], y_pair.at[pl.ds(D, D), :], yx_sem)
    x_swap = send(x_in.at[:, columns(other * HALF, HALF)], x_peer, xx_sem)

    def a_swap(layer, tile):
        src, dst, sem = ((a_one, a_one_peer, a_one_sem), (a_two, a_two_peer, a_two_sem))[layer]
        return send(src.at[:, columns(other * OWN + tile * TILE, TILE)], dst.at[:, columns(tile * TILE, TILE)], sem.at[tile])

    def dh_swap(layer, tile):
        return send(dh_own.at[:, columns(tile * HALF, HALF)], dh_peer.at[:, columns(tile * HALF, HALF)], dh_sem.at[layer, tile])

    def dyp_swap(tile):
        return send(dy_pair.at[pl.ds(0, D), columns(tile * TILE, TILE)], dy_pair.at[pl.ds(D, D), columns(tile * TILE, TILE)], dyp_sem.at[tile])

    def a_load(layer, tile, part):
        slot = lax.rem(tile, BOTH)
        if part == 0:
            src = (a_one, a_two)[layer].at[:, columns(core * OWN + tile * TILE, TILE)]
        else:
            src = (a_one_peer, a_two_peer)[layer].at[:, columns(tile * TILE, TILE)]
        return pltpu.make_async_copy(src, a_tile.at[slot, pl.ds(part * D, D), :], a_tile_sem.at[slot, part])

    def w_load(layer, tile):
        slot = lax.rem(tile, BOTH)
        src = (w_two, w_four)[layer].at[pl.ds(pl.multiple_of(tile * HALF, HALF), HALF), :]
        return [pltpu.make_async_copy(src.at[pl.ds(part * TILE, TILE), :], w_tile.at[slot, :, pl.ds(part * D, D)], w_tile_sem.at[slot, part]) for part in range(2)]

    def w_three_load(tile):
        slot = lax.rem(tile, BOTH)
        return [pltpu.make_async_copy(w_three.at[pl.ds(pl.multiple_of(tile * TILE, TILE), TILE), :], w_tile.at[slot], w_tile_sem.at[slot, 0])]

    def h_load(layer, tile):
        slot = lax.rem(tile, BOTH)
        return pltpu.make_async_copy((h_one, h_two)[layer].at[:, columns(tile * HALF, HALF)], h_tile.at[slot], h_tile_sem.at[slot])

    def start_all(copies):
        for copy in copies:
            copy.start()

    def wait_all(copies):
        for copy in copies:
            copy.wait()

    dy_load = pltpu.make_async_copy(dy_in, dy_pair.at[pl.ds(0, D), :], load_sem.at[0])
    y_load = pltpu.make_async_copy(y_one.at[:, columns(core * HALF, HALF)], y_pair.at[pl.ds(0, D), :], load_sem.at[1])
    x_load = pltpu.make_async_copy(x_in.at[:, columns(core * HALF, HALF)], y_pair.at[pl.ds(0, D), :], load_sem.at[2])
    x_peer_load = pltpu.make_async_copy(x_peer, y_pair.at[pl.ds(D, D), :], load_sem.at[3])

    dy_load.start()
    start_all(w_load(1, 0))
    h_load(1, 0).start()
    a_load(1, 0, 0).start()
    y_load.start()
    ex.greet()
    dy_swap.start()
    for layer in (1, 0):
        def swap_one(tile, carry, layer=layer):
            a_swap(layer, tile).start()
            return carry
        lax.fori_loop(0, TILES, swap_one, 0)
        if layer == 1:
            y_swap.start()
    x_swap.start()
    norm_buf[4, 0] = jnp.zeros((OCT, LANE), F32)
    dy_load.wait()

    def dh_slot(layer, tile):
        slot = lax.rem(tile, BOTH)

        @pl.when(tile < TILES - 1)
        def _():
            start_all(w_load(layer, tile + 1))
            h_load(layer, tile + 1).start()

        if layer == 1:
            @pl.when(tile == TILES - 1)
            def _():
                start_all(w_three_load(0))
        wait_all(w_load(layer, tile))
        h_load(layer, tile).wait()
        def part_body(part, carry):
            rows = pl.ds(pl.multiple_of(part * HALF, HALF), HALF)
            for half in range(2):
                acc = lax.dot_general(dy_pair[rows, :], w_tile[slot, :, half * D:(half + 1) * D], COLS_COLS, preferred_element_type=F32)
                slope = gelu_slope(h_tile[slot, rows, half * TILE:(half + 1) * TILE].astype(F32))
                dh_own[rows, columns(tile * HALF + half * TILE, TILE)] = (slope * acc.astype(jnp.bfloat16).astype(F32)).astype(jnp.bfloat16)
            return carry
        lax.fori_loop(0, BOTH, part_body, 0)
        dh_swap(layer, tile).start()

    def row_slot(layer, tile):
        slot = lax.rem(tile, BOTH)

        @pl.when(tile == 0)
        def _():
            if layer == 1:
                dy_swap.wait()
                y_swap.wait_send()
            else:
                for part in range(4):
                    dyp_swap(part).wait()
            a_swap(layer, tile).wait()
            a_load(layer, tile, 1).start()

        @pl.when(tile < TILES - 1)
        def _():
            a_load(layer, tile + 1, 0).start()
            a_swap(layer, tile + 1).wait()
            a_load(layer, tile + 1, 1).start()
        a_load(layer, tile, 0).wait()
        a_load(layer, tile, 1).wait()
        grads[1 + 2 * layer, pl.ds(pl.multiple_of(tile * TILE, TILE), TILE), :] = lax.dot_general(a_tile[slot], dy_pair[...], ROWS_ROWS, preferred_element_type=F32)

    def column_slot(layer, tile):
        @pl.when(tile == 0)
        def _():
            if layer == 1:
                y_load.wait()
                y_swap.wait_recv()
            else:
                x_load.wait()
                x_peer_load.wait()
        dh_swap(layer, tile).wait()
        cols = columns(tile * HALF, HALF)

        def part_body(part, carry):
            mine = columns(part * TILE, TILE)
            total = lax.dot_general(y_pair[0:D, mine], dh_own[:, cols], ROWS_ROWS, preferred_element_type=F32)
            total = total + lax.dot_general(y_pair[D:BOTH * D, mine], dh_peer[:, cols], ROWS_ROWS, preferred_element_type=F32)
            rows = pl.ds(pl.multiple_of(lax.div(tile, 2) * HALF + part * TILE, TILE), TILE)
            grads[2 * layer, rows, columns(lax.rem(tile, BOTH) * HALF, HALF)] = total
            return carry
        lax.fori_loop(0, BOTH, part_body, 0)

    def dy_slot(tile):
        slot = lax.rem(tile, BOTH)

        @pl.when(tile < 3)
        def _():
            start_all(w_three_load(tile + 1))

        @pl.when(tile == 3)
        def _():
            start_all(w_load(0, 0))
            h_load(0, 0).start()
            a_load(0, 0, 0).start()
            x_load.start()
            x_swap.wait()
            x_peer_load.start()
        wait_all(w_three_load(tile))
        acc = lax.dot_general(dh_own[...], w_tile[slot], COLS_COLS, preferred_element_type=F32)
        dy_pair[0:D, columns(tile * TILE, TILE)] = acc.astype(jnp.bfloat16)
        dyp_swap(tile).start()

    def lane_tile(item, which):
        lane = lax.rem(item, LANES)
        return slot_big.at[lax.div(lane, 6), lax.rem(lax.div(lane, 2), 3), which, lax.rem(lane, 2)]

    def w_stage(item):
        return dh_own.at[piece_rows(lax.rem(item, LANES)), 0:D]

    def state_view(ref, mat, piece):
        if mat in (1, 3):
            return ref.at[piece_rows(piece), :]
        return ref.at[piece_rows(lax.rem(piece, OCT)), columns(lax.div(piece, OCT) * D, D)]

    def w_view(mat, piece):
        ref = new_w[mat]
        if mat in (1, 3):
            return ref.at[piece_rows(piece, core * OWN), :]
        return ref.at[piece_rows(lax.rem(piece, OCT), core * HALF), columns(lax.div(piece, OCT) * D, D)]

    def state_load(item, which, mat, piece):
        return pltpu.make_async_copy(state_view((moms, vels, masters)[which][mat], mat, piece), lane_tile(item, which), in_sem.at[lax.rem(item, LANES), which])

    def state_store(item, which, mat, piece):
        return pltpu.make_async_copy(lane_tile(item, which), state_view((new_moms, new_vels, new_masters)[which][mat], mat, piece), out_sem.at[lax.rem(item, LANES), which])

    def w_store(item, mat, piece):
        return pltpu.make_async_copy(w_stage(item), w_view(mat, piece), out_sem.at[lax.rem(item, LANES), N_STATE])

    def w_swap(item, mat, piece):
        return pltpu.make_async_remote_copy(src_ref=w_stage(item), dst_ref=w_view(mat, piece), send_sem=w_send.at[lax.rem(item, LANES)], recv_sem=w_recv.at[item], device_id=mate, device_id_type=MESH)

    def piece_of(item):
        idx = lax.rem(item, PIECES)
        early = idx < 12
        rest = idx - 12
        stream = jnp.where(early, lax.div(lax.rem(idx, 6), BOTH), lax.div(rest, RING))
        odd = lax.rem(idx, BOTH)
        far = lax.div(lax.rem(rest + 12, RING), BOTH)
        delta = jnp.where(idx < 6, 0, jnp.where(early, 3 - BOTH * odd, jnp.where(far == 1, BOTH, 3 - BOTH * odd)))
        half = jnp.where(early, odd, jnp.where(far == 1, odd, 1 - odd))
        pos = jnp.where(stream == 0, ex.pos[0], jnp.where(stream == 1, ex.pos[1], ex.pos[2]))
        return stream * OCT + lax.rem(pos + delta, RING) * BOTH + half

    def for_mat(item, body):
        place = lax.div(item, PIECES)
        piece = piece_of(item)
        for which in range(NMAT):
            @pl.when(place == which)
            def _(which=which):
                body(NMAT - 1 - which, piece)

    def adam_fetch(item):
        def body(mat, piece):
            for which in range(N_STATE):
                state_load(item, which, mat, piece).start()
        for_mat(item, body)

    def adam_flush(item):
        for which in range(N_STATE):
            state_store(item, which, 1, 0).wait()
        w_store(item, 1, 0).wait()
        w_swap(item, 1, 0).wait_send()

    def adam_item(item):
        @pl.when(item >= LANES - AHEAD)
        def _():
            adam_flush(item - (LANES - AHEAD))

        @pl.when(item < NMAT * PIECES - AHEAD)
        def _():
            adam_fetch(item + AHEAD)
        for which in range(N_STATE):
            state_load(item, which, 1, 0).wait()
        mom, vel, master = (lane_tile(item, which) for which in range(N_STATE))
        mat, piece = NMAT - 1 - lax.div(item, PIECES), piece_of(item)
        scaled = scale_ref[0:1, 0:1] * grads[mat, piece_rows(piece), :]
        mom_new = BETA_ONE * mom[...] + (1.0 - BETA_ONE) * scaled
        vel_new = BETA_TWO * vel[...] + (1.0 - BETA_TWO) * jnp.square(scaled)
        master_new = master[...] - STEP_SIZE * mom_new / (jnp.sqrt(vel_new * VEL_GAIN) + ADAM_EPS)
        mom[...] = mom_new
        vel[...] = vel_new
        master[...] = master_new
        w_stage(item)[...] = master_new.astype(jnp.bfloat16)

        def body(mat, piece):
            for which in range(N_STATE):
                state_store(item, which, mat, piece).start()
            w_store(item, mat, piece).start()
            w_swap(item, mat, piece).start()
        for_mat(item, body)

    def set_scale():
        total = jnp.sum(jnp.sum(norm_buf[NMAT, NMAT], axis=0, keepdims=True), axis=1, keepdims=True)
        norm = jnp.sqrt(total)
        norm_ref[...] = jnp.broadcast_to(norm, norm_ref.shape)
        scale_ref[...] = jnp.broadcast_to(jnp.minimum(1.0, clip_ref[...] / (norm + NORM_EPS)), scale_ref.shape)

    def during(first, last, now, body):
        @pl.when((now >= first) & (now < last))
        def _():
            body()

    def compute(now):
        during(0, 2, now, lambda: dh_slot(1, now))
        during(2, 8, now, lambda: row_slot(1, now - 2))
        during(8, 12, now, lambda: dh_slot(1, now - 6))
        during(12, 18, now, lambda: column_slot(1, now - 12))
        during(18, 22, now, lambda: dy_slot(now - 18))
        during(22, 28, now, lambda: row_slot(0, now - 22))
        during(28, 34, now, lambda: dh_slot(0, now - 28))
        during(34, 40, now, lambda: column_slot(0, now - 34))

    def late(now):
        for stage in range(NMAT + 1):
            @pl.when(now == NORM_SLOTS[stage])
            def _(stage=stage):
                if stage > 0:
                    ex.norm_finish(stage - 1)
                if stage < NMAT:
                    ex.norm_start(stage)
                else:
                    set_scale()

        @pl.when(now == ADAM_READY)
        def _():
            for item in range(AHEAD):
                adam_fetch(item)

        first = 0
        active = 0
        for start, length, chunk in ADAM_RUNS:
            inside = (now >= start) & (now < start + length)
            first = jnp.where(inside, (now - start + chunk) * PER_SLOT, first)
            active = jnp.where(inside, 1, active)

        @pl.when(active == 1)
        def _():
            def adam_body(idx, carry):
                adam_item(first + idx)
                return carry
            lax.fori_loop(0, PER_SLOT, adam_body, 0)

    def slot_body(now, carry):
        @pl.when(now < COMPUTE_SLOTS)
        def _():
            compute(now)

        nums = []
        for which in range(NMAT):
            num = -1
            for order, at in enumerate(STEP_SLOTS[which]):
                num = jnp.where(now == at, order, num)
            nums.append(num)

        def place_body(place, c2):
            num = nums[0]
            for which in range(1, NMAT):
                num = jnp.where(place == which, nums[which], num)
            mat = NMAT - 1 - place

            @pl.when(num >= 0)
            def _():
                for want in range(13):
                    @pl.when(num == want)
                    def _(want=want):
                        ex.step(mat, want)
            return c2
        most = jnp.maximum(jnp.maximum(nums[0], nums[1]), jnp.maximum(nums[2], nums[3]))

        @pl.when(most >= 0)
        def _():
            lax.fori_loop(0, NMAT, place_body, 0)

        @pl.when(now >= COMPUTE_SLOTS)
        def _():
            late(now)
        return carry

    lax.fori_loop(0, SLOTS, slot_body, 0)
    for item in range(NMAT * PIECES - (LANES - AHEAD), NMAT * PIECES):
        adam_flush(item)

    def w_wait(item, carry):
        w_swap(item, 1, 0).wait_recv()
        return carry
    lax.fori_loop(0, NMAT * PIECES, w_wait, 0)
    ex.drain()


def backward(acts, clip_norm, masters, moms, vels):
    bf16 = jnp.bfloat16
    sds = jax.ShapeDtypeStruct
    dma = pltpu.SemaphoreType.DMA
    whole = [sds((D, FF), bf16), sds((FF, D), bf16)]
    rows = [sds((HALF, FF), F32), sds((OWN, D), F32)]
    in_vmem = pl.BlockSpec(memory_space=pltpu.VMEM)
    outs = pl.pallas_call(
        backward_kernel,
        out_shape=whole * 2 + rows * 6 + [sds((OCT, LANE), F32), sds((D, HALF), bf16), sds((D, OWN), bf16), sds((D, OWN), bf16)],
        in_specs=[HBM_ANY] * (N_ACTS - 1) + [in_vmem] + [HBM_ANY] * (N_STATE * NMAT),
        out_specs=[HBM_ANY] * (NMAT * NMAT) + [in_vmem] + [HBM_ANY] * N_STATE,
        scratch_shapes=[
            pltpu.VMEM((NMAT, OWN, D), F32),
            pltpu.VMEM((NSET, AXES, AXES, BOTH) + HALF_SHAPE[0], F32),
            pltpu.VMEM((NSET, AXES, AXES, BOTH) + HALF_SHAPE[1], F32),
            pltpu.VMEM((NSET, AXES, AXES, BOTH) + HALF_SHAPE[2], F32),
            pltpu.VMEM((NMAT + 1, NMAT + 1, OCT, LANE), F32),
            pltpu.VMEM((OCT, LANE), F32),
            pltpu.VMEM((D, FF), bf16),
            pltpu.VMEM((D, FF), bf16),
            pltpu.VMEM((BOTH * D, D), bf16),
            pltpu.VMEM((BOTH * D, HALF), bf16),
            pltpu.VMEM((2, BOTH * D, TILE), bf16),
            pltpu.VMEM((2, TILE, FF), bf16),
            pltpu.VMEM((2, D, HALF), bf16),
            dma((NMAT, AXES)),
            dma((NMAT, AXES, BOTH)),
            dma((NMAT, AXES)),
            dma((NMAT, AXES, BOTH)),
            pltpu.SemaphoreType.REGULAR((NMAT, AXES)),
            pltpu.SemaphoreType.REGULAR((NMAT, AXES)),
            dma((4, 4)),
            dma((4, 4)),
            dma((2, 2)),
            dma((2, 3)),
            dma((BOTH,)),
            dma((4,)),
            dma((BOTH,)),
            dma((BOTH,)),
            dma((BOTH,)),
            dma((TILES, BOTH)),
            dma((TILES, BOTH)),
            dma((2, 6, 2)),
            dma((4, 2)),
            dma((LANES, 3)),
            dma((LANES, 4)),
            dma((LANES,)),
            dma((NMAT * PIECES,)),
        ],
        compiler_params=pltpu.CompilerParams(collective_id=0, has_side_effects=True, vmem_limit_bytes=67043328),
        name='backward_exchange',
    )(*acts, clip_norm.reshape(1, 1), *masters, *moms, *vels)
    return outs[:NMAT * NMAT], outs[NMAT * NMAT]


def gelu_fn(values):
    return jax.nn.gelu(values, approximate=True)


def forward(act_in, w_one, w_two, w_three):
    bf16 = jnp.bfloat16
    h_one = jnp.dot(act_in, w_one, preferred_element_type=F32).astype(bf16)
    a_one = gelu_fn(h_one.astype(F32)).astype(bf16)
    y_one = jnp.dot(a_one, w_two, preferred_element_type=F32).astype(bf16)
    h_two = jnp.dot(y_one, w_three, preferred_element_type=F32).astype(bf16)
    a_two = gelu_fn(h_two.astype(F32)).astype(bf16)
    return h_one, a_one, y_one, h_two, a_two


def solution(mesh):
    row_spec = P(('rep', 'data'), None)
    shard_spec = P('data', None)
    full_spec = P()

    def per_device(act_in, grad_out, w_one, w_two, w_three, w_four, master_one, master_two, master_three, master_four, mom_one, mom_two, mom_three, mom_four, vel_one, vel_two, vel_three, vel_four, clip_norm):
        h_one, a_one, y_one, h_two, a_two = forward(act_in, w_one, w_two, w_three)
        acts = (act_in, grad_out, w_two, w_three, w_four, h_one, a_one, y_one, h_two, a_two)
        new_state, norm_block = backward(acts, clip_norm, (master_one, master_two, master_three, master_four), (mom_one, mom_two, mom_three, mom_four), (vel_one, vel_two, vel_three, vel_four))
        return tuple(new_state) + (norm_block[0, 0],)

    in_specs = (row_spec, row_spec, full_spec, full_spec, full_spec, full_spec) + (shard_spec,) * 12 + (full_spec,)
    out_specs = (full_spec,) * 4 + (shard_spec,) * 12 + (full_spec,)
    return jax.shard_map(per_device, mesh=mesh, in_specs=in_specs, out_specs=out_specs, check_vma=False)
```

```python
import jax
import jax.numpy as jnp
from jax import lax
from jax.experimental import pallas as pl
from jax.experimental.pallas import tpu as pltpu
from jax.sharding import PartitionSpec as P

TRAIN_STEP = 10
BETA_ONE = 0.9
BETA_TWO = 0.95
ADAM_EPS = 1e-8
NORM_EPS = 1e-6
LEARN_RATE = 0.003
STEP_SIZE = LEARN_RATE / (1.0 - BETA_ONE ** TRAIN_STEP)
VEL_GAIN = 1.0 / (1.0 - BETA_TWO ** TRAIN_STEP)
MESH = pl.DeviceIdType.MESH
NMAT = 4
F32 = jnp.float32
D = 1024
FF = 3072
HALF = 512
TILE = 256
HALF_SHAPE = ((64, 1024), (16, 1024), (8, 512))
CHUNK_ROWS = (128, 32, 8)
AXES = 3
RING = 4
BOTH = 2
NSET = 2


class Torus:
    def __init__(self):
        self.rep = lax.axis_index('rep')
        self.core = lax.axis_index('data')

    def stride(self, axis):
        return 1 + 3 * lax.rem(axis, 3) + 9 * lax.div(lax.rem(axis, 3), 2)

    def pos(self, axis):
        return lax.rem(lax.div(self.rep, self.stride(axis)), 4)

    def peer(self, axis, delta):
        stride = self.stride(axis)
        pos = lax.rem(lax.div(self.rep, stride), 4)
        return {'rep': self.rep + (lax.rem(pos + delta + 4, 4) - pos) * stride, 'data': self.core}


class Exchange:
    def __init__(self, tor, grads, slots, norm_buf, rs_send, rs_recv, ag_send, ag_recv, free_sem, slot_sem, nm_send, nm_recv):
        self.free_sem, self.slot_sem = free_sem, slot_sem
        self.tor, self.grads, self.slots = tor, grads, slots
        self.pos = [tor.pos(axis) for axis in range(AXES)]
        self.base = []
        for stream in range(AXES):
            base = stream * HALF
            for level in range(AXES):
                self.base.append(base)
                base = base + self.pos[(stream + level) % AXES] * CHUNK_ROWS[level]
        self.norm_buf = norm_buf
        self.rs_send, self.rs_recv, self.ag_send, self.ag_recv = rs_send, rs_recv, ag_send, ag_recv
        self.nm_send, self.nm_recv = nm_send, nm_recv

    def neighbour(self, stream, level, side):
        axis = (stream + level) % AXES
        pos = self.pos[axis]
        return {'rep': self.tor.rep + (lax.rem(pos + 1 + BOTH * side, RING) - pos) * RING ** axis, 'data': self.tor.core}

    def region(self, mat, stream, level, delta, half):
        rows = CHUNK_ROWS[level]
        row = self.base[stream * AXES + level] + lax.rem(self.pos[(stream + level) % AXES] + delta, RING) * rows
        if level < BOTH:
            row = pl.multiple_of(row + half * (rows // BOTH), rows // BOTH)
            return self.grads.at[mat, pl.ds(row, rows // BOTH), :]
        return self.grads.at[mat, pl.ds(pl.multiple_of(row, rows), rows), pl.ds(pl.multiple_of(half * HALF, HALF), HALF)]

    def rs_copy(self, mat, stream, level, msg, side):
        near = 1 + BOTH * side
        if isinstance(msg, int):
            delta, half = ((BOTH, side), (near, 1 - side), (near, side))[msg]
        else:
            delta, half = BOTH + msg * (near - BOTH), side + msg * (1 - BOTH * side)
        return pltpu.make_async_remote_copy(
            src_ref=self.region(mat, stream, level, delta, half),
            dst_ref=self.slots[level].at[lax.rem(mat, NSET), stream, msg, side],
            send_sem=self.rs_send.at[mat, level],
            recv_sem=self.rs_recv.at[mat, level, msg - msg // BOTH if isinstance(msg, int) else msg],
            device_id=self.neighbour(stream, level, side), device_id_type=MESH)

    def ag_copy(self, mat, stream, level, msg, side):
        if isinstance(msg, int):
            delta, half = ((0, side), (0, 1 - side), (RING - 1 - BOTH * side, side))[msg]
        else:
            delta, half = 0, side + msg * (1 - BOTH * side)
        ref = self.region(mat, stream, level, delta, half)
        return pltpu.make_async_remote_copy(
            src_ref=ref, dst_ref=ref,
            send_sem=self.ag_send.at[mat, level],
            recv_sem=self.ag_recv.at[mat, level, msg - msg // BOTH if isinstance(msg, int) else msg],
            device_id=self.neighbour(stream, level, side), device_id_type=MESH)

    def pairs(self, body, msgs=1):
        for stream in range(AXES):
            def one(idx, carry, stream=stream):
                body(stream, lax.rem(idx, BOTH), lax.div(idx, BOTH))
                return carry
            lax.fori_loop(0, BOTH * msgs, one, 0)

    def bulk(self, mat, level, late, gather):
        send, recv = (self.ag_send, self.ag_recv) if gather else (self.rs_send, self.rs_recv)
        count = AXES * BOTH * (AXES if late is None else 1 + late)
        rows = count * HALF_SHAPE[level][0] * HALF_SHAPE[level][1] // D
        ref = self.grads.at[mat, pl.ds(0, rows), :]
        copy = pltpu.make_async_remote_copy(src_ref=ref, dst_ref=ref, send_sem=send.at[mat, level], recv_sem=recv.at[mat, level, late or 0], device_id=self.neighbour(0, level, 0), device_id_type=MESH)
        if late is None:
            copy.wait_send()
        else:
            copy.wait_recv()

    def rs_first(self, mat, level):
        @pl.when(mat < NMAT - NSET)
        def _():
            pl.semaphore_wait(self.slot_sem.at[mat, level], AXES * BOTH)
        self.pairs(lambda stream, side, msg: self.rs_copy(mat, stream, level, msg, side).start(), BOTH)

    def rs_mid(self, mat, level):
        self.bulk(mat, level, 0, False)

        def body(stream, side, _):
            ref = self.region(mat, stream, level, 1 + BOTH * side, side)
            ref[...] = ref[...] + self.slots[level][lax.rem(mat, NSET), stream, 0, side]
            self.rs_copy(mat, stream, level, BOTH, side).start()
        self.pairs(body)

    def rs_last(self, mat, level):
        self.bulk(mat, level, 1, False)
        self.bulk(mat, level, None, False)

        def body(stream, half, _):
            ref = self.region(mat, stream, level, 0, half)
            held = self.slots[level]
            total = ref[...] + held[lax.rem(mat, NSET), stream, 2, half] + held[lax.rem(mat, NSET), stream, 1, 1 - half]
            if level == 2:
                total = total * (1.0 / 128.0)
                square = total * total
                self.norm_buf[4, 0] = self.norm_buf[4, 0] + sum(square[:, col * 128:(col + 1) * 128] for col in range(RING))
            ref[...] = total
        self.pairs(body)

        def tell(stream, side, _):
            peer = self.neighbour(stream, level, side)
            pl.semaphore_signal(self.free_sem.at[mat, level], inc=1, device_id=peer, device_id_type=MESH)

            @pl.when(mat >= NSET)
            def _():
                pl.semaphore_signal(self.slot_sem.at[mat - NSET, level], inc=1, device_id=peer, device_id_type=MESH)
        self.pairs(tell)

    def ag_first(self, mat, level):
        pl.semaphore_wait(self.free_sem.at[mat, level], AXES * BOTH)
        self.pairs(lambda stream, side, msg: self.ag_copy(mat, stream, level, msg, side).start(), BOTH)

    def ag_mid(self, mat, level):
        self.bulk(mat, level, 0, True)
        self.pairs(lambda stream, side, _: self.ag_copy(mat, stream, level, BOTH, side).start())

    def ag_last(self, mat, level):
        self.bulk(mat, level, 1, True)

    def step(self, mat, num):
        if num == 0:
            self.rs_first(mat, 0)
        elif num in (1, 3, 5):
            self.rs_mid(mat, num // 2)
        elif num in (2, 4):
            self.rs_last(mat, num // 2 - 1)
            self.rs_first(mat, num // 2)
        elif num == 6:
            self.rs_last(mat, 2)
            self.ag_first(mat, 2)
        elif num in (7, 9, 11):
            self.ag_mid(mat, 2 - (num - 7) // 2)
        elif num in (8, 10):
            level = 2 - (num - 8) // 2
            self.ag_last(mat, level)
            self.ag_first(mat, level - 1)
        else:
            self.ag_last(mat, 0)
            for level in range(AXES):
                self.bulk(mat, level, None, True)

    def norm_copy(self, stage, delta):
        tor = self.tor
        if stage < 3:
            mine, dev = tor.pos(stage), tor.peer(stage, delta)
        else:
            mine, dev = tor.core, {'data': 1 - tor.core}
        return pltpu.make_async_remote_copy(
            src_ref=self.norm_buf.at[4, stage], dst_ref=self.norm_buf.at[stage, mine],
            send_sem=self.nm_send.at[stage, delta], recv_sem=self.nm_recv.at[stage, delta],
            device_id=dev, device_id_type=MESH)

    def deltas(self, stage):
        return (1, 2, 3) if stage < AXES else (1,)

    def norm_start(self, stage):
        for delta in (self.deltas(stage)):
            self.norm_copy(stage, delta).start()
        mine = self.tor.pos(stage) if stage < 3 else self.tor.core
        self.norm_buf[stage, mine] = self.norm_buf[4, stage]

    def norm_finish(self, stage):
        for delta in (self.deltas(stage)):
            self.norm_copy(stage, delta).wait_recv()
        total = self.norm_buf[stage, 0] + self.norm_buf[stage, 1]
        if stage < 3:
            total = total + self.norm_buf[stage, 2] + self.norm_buf[stage, 3]
            self.norm_buf[4, stage + 1] = total
        else:
            self.norm_buf[4, 4] = total

    def drain(self):
        for stage in range(4):
            for delta in (self.deltas(stage)):
                self.norm_copy(stage, delta).wait_send()

    def greet(self):
        tor = self.tor
        barrier = pltpu.get_barrier_semaphore()
        for axis in range(AXES):
            for delta in (1, 2, 3):
                pl.semaphore_signal(barrier, inc=1, device_id=tor.peer(axis, delta), device_id_type=MESH)
        pl.semaphore_signal(barrier, inc=1, device_id={'data': 1 - tor.core}, device_id_type=MESH)
        return barrier


SUB = 64
OCT = 8
LANE = 128
OWN = 1536
TILES = 6
HBM_ANY = pl.BlockSpec(memory_space=pl.ANY)
ROWS_ROWS = (((0,), (0,)), ((), ()))
COLS_COLS = (((1,), (1,)), ((), ()))
COMPUTE_SLOTS = 40
FIRST_SWAP = 2
STEP_SLOTS = (
    (9, 14, 20, 25, 28, 37, 41, 43, 46, 48, 49, 51, 55),
    (18, 21, 27, 30, 36, 40, 43, 45, 48, 51, 54, 58, 66),
    (28, 33, 37, 42, 44, 47, 48, 50, 52, 56, 61, 71, 80),
    (39, 41, 43, 46, 48, 49, 51, 55, 61, 75, 81, 90, 98),
)
NORM_SLOTS = (52, 53, 54, 55, 56)
ADAM_RUNS = ((56, 48, 0),)
ADAM_READY = 44
LANES = 12
AHEAD = 8
PER_SLOT = 2
PIECES = 24
SLOTS = 104
GELU_A = 0.7978845608028654
GELU_B = 0.044715


def gelu_slope(hidden):
    square = hidden * hidden
    tanh = jnp.tanh(hidden * (GELU_A + GELU_A * GELU_B * square))
    return 0.5 * (1.0 + tanh) + (0.5 * hidden) * (1.0 - tanh * tanh) * (GELU_A + 3.0 * GELU_A * GELU_B * square)


N_ACTS = 11
N_STATE = 3
N_LATE = 7
LAST = (NMAT - 1) * PIECES
SCOPED_BYTES = 67043328 - (NMAT * OWN * D * 4 + 2 * D * FF * 2)


def take(refs, count, start=0):
    return refs[start:start + count]


def backward_kernel(*refs):
    x_in, dy_in, w_two, w_three, w_four, h_one, a_one, y_one, h_two, a_two, clip_ref = take(refs, N_ACTS)
    masters, moms, vels = (take(refs, NMAT, N_ACTS + which * NMAT) for which in range(N_STATE))
    outs = refs[N_ACTS + N_STATE * NMAT:]
    mate_w, new_masters, new_vels = (take(outs, NMAT, which * NMAT) for which in range(N_STATE))
    grads, dh_pair, last_mom, norm_ref, x_peer, a_one_peer, a_two_peer = take(outs, N_LATE, N_STATE * NMAT)
    (slot_big, slot_mid, slot_low, norm_buf, scale_ref, dy_pair, y_pair, a_tile, w_tile, h_tile,
     rs_send, rs_recv, ag_send, ag_recv, free_sem, slot_sem, nm_send, nm_recv,
     a_tile_sem, w_tile_sem, h_tile_sem, load_sem, dyx_sem, yx_sem, xx_sem, a_one_sem, a_two_sem, dh_sem, dyp_sem,
     in_sem, out_sem, w_send, w_recv) = outs[N_STATE * NMAT + N_LATE:]
    dh_own, dh_peer = dh_pair.at[0], dh_pair.at[1]
    tor = Torus()
    ex = Exchange(tor, grads, (slot_big, slot_mid, slot_low), norm_buf, rs_send, rs_recv, ag_send, ag_recv, free_sem, slot_sem, nm_send, nm_recv)
    core = tor.core
    other = 1 - core
    mate = {'data': other}

    def send(src, dst, sem):
        return pltpu.make_async_remote_copy(src_ref=src, dst_ref=dst, send_sem=sem.at[0], recv_sem=sem.at[1], device_id=mate, device_id_type=MESH)

    def columns(start, size):
        return pl.ds(pl.multiple_of(start, size), size)

    def piece_rows(index, base=0):
        return pl.ds(pl.multiple_of(base + index * SUB, SUB), SUB)

    dy_swap = send(dy_in, dy_pair.at[pl.ds(D, D), :], dyx_sem)
    y_swap = send(y_one.at[:, columns(other * HALF, HALF)], y_pair.at[pl.ds(D, D), :], yx_sem)
    x_swap = send(x_in.at[:, columns(other * HALF, HALF)], x_peer, xx_sem)

    def a_swap(layer, tile):
        src, dst, sem = ((a_one, a_one_peer, a_one_sem), (a_two, a_two_peer, a_two_sem))[layer]
        return send(src.at[:, columns(other * OWN + tile * TILE, TILE)], dst.at[:, columns(tile * TILE, TILE)], sem.at[tile])

    def dh_swap(layer, tile):
        return send(dh_own.at[:, columns(tile * HALF, HALF)], dh_peer.at[:, columns(tile * HALF, HALF)], dh_sem.at[layer, tile])

    def dyp_swap(tile):
        return send(dy_pair.at[pl.ds(0, D), columns(tile * TILE, TILE)], dy_pair.at[pl.ds(D, D), columns(tile * TILE, TILE)], dyp_sem.at[tile])

    def a_load(layer, tile, part):
        slot = lax.rem(tile, BOTH)
        if part == 0:
            src = (a_one, a_two)[layer].at[:, columns(core * OWN + tile * TILE, TILE)]
        else:
            src = (a_one_peer, a_two_peer)[layer].at[:, columns(tile * TILE, TILE)]
        return pltpu.make_async_copy(src, a_tile.at[slot, pl.ds(part * D, D), :], a_tile_sem.at[slot, part])

    def w_load(layer, tile):
        slot = lax.rem(tile, BOTH)
        src = (w_two, w_four)[layer].at[pl.ds(pl.multiple_of(tile * HALF, HALF), HALF), :]
        return [pltpu.make_async_copy(src.at[pl.ds(part * TILE, TILE), :], w_tile.at[slot, :, pl.ds(part * D, D)], w_tile_sem.at[slot, part]) for part in range(2)]

    def w_three_load(tile):
        slot = lax.rem(tile, BOTH)
        return [pltpu.make_async_copy(w_three.at[pl.ds(pl.multiple_of(tile * TILE, TILE), TILE), :], w_tile.at[slot], w_tile_sem.at[slot, 0])]

    def h_load(layer, tile):
        slot = lax.rem(tile, BOTH)
        return pltpu.make_async_copy((h_one, h_two)[layer].at[:, columns(tile * HALF, HALF)], h_tile.at[slot], h_tile_sem.at[slot])

    def start_all(copies):
        for copy in copies:
            copy.start()

    def wait_all(copies):
        for copy in copies:
            copy.wait()

    dy_load = pltpu.make_async_copy(dy_in, dy_pair.at[pl.ds(0, D), :], load_sem.at[0])
    y_load = pltpu.make_async_copy(y_one.at[:, columns(core * HALF, HALF)], y_pair.at[pl.ds(0, D), :], load_sem.at[1])
    x_load = pltpu.make_async_copy(x_in.at[:, columns(core * HALF, HALF)], y_pair.at[pl.ds(0, D), :], load_sem.at[2])
    x_peer_load = pltpu.make_async_copy(x_peer, y_pair.at[pl.ds(D, D), :], load_sem.at[3])

    dy_load.start()
    start_all(w_load(1, 0))
    h_load(1, 0).start()
    a_load(1, 0, 0).start()
    y_load.start()
    barrier = ex.greet()
    norm_buf[4, 0] = jnp.zeros((OCT, LANE), F32)
    dy_load.wait()

    def first_swaps():
        pl.semaphore_wait(barrier, 10)
        dy_swap.start()
        for layer in (1, 0):
            def swap_one(tile, carry, layer=layer):
                a_swap(layer, tile).start()
                return carry
            lax.fori_loop(0, TILES, swap_one, 0)
            if layer == 1:
                y_swap.start()
        for tile in range(FIRST_SWAP):
            dh_swap(1, tile).start()
        x_swap.start()

    def dh_slot(layer, tile):
        slot = lax.rem(tile, BOTH)

        @pl.when(tile < TILES - 1)
        def _():
            start_all(w_load(layer, tile + 1))
            h_load(layer, tile + 1).start()

        if layer == 1:
            @pl.when(tile == TILES - 1)
            def _():
                start_all(w_three_load(0))
        wait_all(w_load(layer, tile))
        h_load(layer, tile).wait()
        def part_body(part, carry):
            rows = pl.ds(pl.multiple_of(part * HALF, HALF), HALF)
            for half in range(2):
                acc = lax.dot_general(dy_pair[rows, :], w_tile[slot, :, half * D:(half + 1) * D], COLS_COLS, preferred_element_type=F32)
                slope = gelu_slope(h_tile[slot, rows, half * TILE:(half + 1) * TILE].astype(F32))
                dh_own[rows, columns(tile * HALF + half * TILE, TILE)] = (slope * acc.astype(jnp.bfloat16).astype(F32)).astype(jnp.bfloat16)
            return carry
        lax.fori_loop(0, BOTH, part_body, 0)
        if layer == 1:
            @pl.when(tile >= FIRST_SWAP)
            def _():
                dh_swap(layer, tile).start()
        else:
            dh_swap(layer, tile).start()

    def row_slot(layer, tile):
        slot = lax.rem(tile, BOTH)

        @pl.when(tile == 0)
        def _():
            if layer == 1:
                dy_swap.wait()
                y_swap.wait_send()
            else:
                for part in range(4):
                    dyp_swap(part).wait()
            a_swap(layer, tile).wait()
            a_load(layer, tile, 1).start()

        @pl.when(tile < TILES - 1)
        def _():
            a_load(layer, tile + 1, 0).start()
            a_swap(layer, tile + 1).wait()
            a_load(layer, tile + 1, 1).start()
        a_load(layer, tile, 0).wait()
        a_load(layer, tile, 1).wait()
        grads[1 + 2 * layer, pl.ds(pl.multiple_of(tile * TILE, TILE), TILE), :] = lax.dot_general(a_tile[slot], dy_pair[...], ROWS_ROWS, preferred_element_type=F32)

    def column_slot(layer, tile):
        @pl.when(tile == 0)
        def _():
            if layer == 1:
                y_load.wait()
                y_swap.wait_recv()
            else:
                x_load.wait()
                x_peer_load.wait()
        dh_swap(layer, tile).wait()
        cols = columns(tile * HALF, HALF)

        total = lax.dot_general(y_pair[0:D, :], dh_own[:, cols], ROWS_ROWS, preferred_element_type=F32)
        total = total + lax.dot_general(y_pair[D:BOTH * D, :], dh_peer[:, cols], ROWS_ROWS, preferred_element_type=F32)
        rows = pl.ds(pl.multiple_of(lax.div(tile, BOTH) * HALF, HALF), HALF)
        grads[2 * layer, rows, columns(lax.rem(tile, BOTH) * HALF, HALF)] = total

    def dy_slot(tile):
        slot = lax.rem(tile, BOTH)

        @pl.when(tile < 3)
        def _():
            start_all(w_three_load(tile + 1))

        @pl.when(tile == 3)
        def _():
            start_all(w_load(0, 0))
            h_load(0, 0).start()
            a_load(0, 0, 0).start()
            x_load.start()
            x_swap.wait()
            x_peer_load.start()
        wait_all(w_three_load(tile))

        def part_body(part, carry):
            rows = pl.ds(pl.multiple_of(part * HALF, HALF), HALF)
            acc = lax.dot_general(dh_own[rows, :], w_tile[slot], COLS_COLS, preferred_element_type=F32)
            dy_pair[rows, columns(tile * TILE, TILE)] = acc.astype(jnp.bfloat16)
            return carry
        lax.fori_loop(0, BOTH, part_body, 0)
        dyp_swap(tile).start()

    def lane_tile(item, which):
        lane = lax.rem(item, LANES)
        return slot_big.at[lax.div(lane, 6), lax.rem(lax.div(lane, 2), 3), which, lax.rem(lane, 2)]

    def w_stage(mat, piece):
        part = lax.rem(mat, BOTH) * AXES + lax.div(piece, OCT)
        return dh_pair.at[lax.div(mat, BOTH), piece_rows(lax.rem(piece, OCT), lax.rem(part, BOTH) * HALF), columns(lax.div(part, BOTH) * D, D)]

    def state_view(ref, mat, piece):
        if mat in (1, 3):
            return ref.at[piece_rows(piece), :]
        return ref.at[piece_rows(lax.rem(piece, OCT)), columns(lax.div(piece, OCT) * D, D)]

    def state_load(item, which, mat, piece):
        return pltpu.make_async_copy(state_view((moms, vels, masters)[which][mat], mat, piece), lane_tile(item, which), in_sem.at[lax.rem(item, LANES), which])

    def state_store(item, which, mat, piece):
        target = last_mom if which == 0 else (new_vels, new_masters)[which - 1][mat]
        return pltpu.make_async_copy(lane_tile(item, which), state_view(target, mat, piece), out_sem.at[lax.rem(item, LANES), which])

    def w_swap(item, mat, piece):
        return pltpu.make_async_remote_copy(src_ref=w_stage(mat, piece), dst_ref=state_view(mate_w[mat], mat, piece), send_sem=w_send.at[0], recv_sem=w_recv.at[0], device_id=mate, device_id_type=MESH)

    def piece_of(item):
        idx = lax.rem(item, PIECES)
        early = idx < 12
        rest = idx - 12
        stream = jnp.where(early, lax.div(lax.rem(idx, 6), BOTH), lax.div(rest, RING))
        odd = lax.rem(idx, BOTH)
        far = lax.div(lax.rem(rest + 12, RING), BOTH)
        delta = jnp.where(idx < 6, 0, jnp.where(early, 3 - BOTH * odd, jnp.where(far == 1, BOTH, 3 - BOTH * odd)))
        half = jnp.where(early, odd, jnp.where(far == 1, odd, 1 - odd))
        pos = jnp.where(stream == 0, ex.pos[0], jnp.where(stream == 1, ex.pos[1], ex.pos[2]))
        return stream * OCT + lax.rem(pos + delta, RING) * BOTH + half

    def for_mat(item, body):
        place = lax.div(item, PIECES)
        piece = piece_of(item)
        for which in range(NMAT):
            @pl.when(place == which)
            def _(which=which):
                body(NMAT - 1 - which, piece)

    def adam_fetch(item):
        def body(mat, piece):
            for which in range(N_STATE):
                state_load(item, which, mat, piece).start()
        for_mat(item, body)

    def adam_flush(item):
        for which in (1, 2):
            state_store(item, which, 1, 0).wait()

        @pl.when(item >= LAST)
        def _():
            state_store(item, 0, 0, 0).wait()

    def adam_item(item):
        @pl.when(item >= LANES - AHEAD)
        def _():
            adam_flush(item - (LANES - AHEAD))

        @pl.when(item < NMAT * PIECES - AHEAD)
        def _():
            adam_fetch(item + AHEAD)
        for which in range(N_STATE):
            state_load(item, which, 1, 0).wait()
        mom, vel, master = (lane_tile(item, which) for which in range(N_STATE))
        mat, piece = NMAT - 1 - lax.div(item, PIECES), piece_of(item)
        scaled = scale_ref[0:1, 0:1] * grads[mat, piece_rows(piece), :]
        mom_new = BETA_ONE * mom[...] + (1.0 - BETA_ONE) * scaled
        vel_new = BETA_TWO * vel[...] + (1.0 - BETA_TWO) * jnp.square(scaled)
        master_new = master[...] - STEP_SIZE * mom_new / (jnp.sqrt(vel_new * VEL_GAIN) + ADAM_EPS)
        vel[...] = vel_new
        master[...] = master_new

        mom[...] = mom_new
        w_stage(mat, piece)[...] = master_new.astype(jnp.bfloat16)

        @pl.when(item < LAST)
        def _():
            grads[mat, piece_rows(piece), :] = mom[...]

        def body(mat, piece):
            for which in range(N_STATE):
                if which > 0 or mat == 0:
                    state_store(item, which, mat, piece).start()
            w_swap(item, mat, piece).start()
        for_mat(item, body)

    def set_scale():
        total = jnp.sum(jnp.sum(norm_buf[NMAT, NMAT], axis=0, keepdims=True), axis=1, keepdims=True)
        norm = jnp.sqrt(total)
        norm_ref[...] = jnp.broadcast_to(norm, norm_ref.shape)
        scale_ref[...] = jnp.broadcast_to(jnp.minimum(1.0, clip_ref[...] / (norm + NORM_EPS)), scale_ref.shape)

    def during(first, last, now, body):
        @pl.when((now >= first) & (now < last))
        def _():
            body()

    def compute(now):
        during(0, 4, now, lambda: dh_slot(1, now))
        during(4, 10, now, lambda: row_slot(1, now - 4))
        during(10, 12, now, lambda: dh_slot(1, now - TILES))
        during(12, 18, now, lambda: column_slot(1, now - 12))
        during(18, 22, now, lambda: dy_slot(now - 18))
        during(22, 28, now, lambda: row_slot(0, now - 22))
        during(28, 34, now, lambda: dh_slot(0, now - 28))
        during(34, 40, now, lambda: column_slot(0, now - 34))

    def late(now):
        for stage in range(NMAT + 1):
            @pl.when(now == NORM_SLOTS[stage])
            def _(stage=stage):
                if stage > 0:
                    ex.norm_finish(stage - 1)
                if stage < NMAT:
                    ex.norm_start(stage)
                else:
                    set_scale()

        @pl.when(now == ADAM_READY)
        def _():
            for item in range(AHEAD):
                adam_fetch(item)

        first = 0
        active = 0
        for start, length, chunk in ADAM_RUNS:
            inside = (now >= start) & (now < start + length)
            first = jnp.where(inside, (now - start + chunk) * PER_SLOT, first)
            active = jnp.where(inside, 1, active)

        @pl.when(active == 1)
        def _():
            def adam_body(idx, carry):
                adam_item(first + idx)
                return carry
            lax.fori_loop(0, PER_SLOT, adam_body, 0)

    def slot_body(now, carry):
        @pl.when(now == FIRST_SWAP)
        def _():
            first_swaps()

        @pl.when(now < COMPUTE_SLOTS)
        def _():
            compute(now)

        nums = []
        for which in range(NMAT):
            num = -1
            for order, at in enumerate(STEP_SLOTS[which]):
                num = jnp.where(now == at, order, num)
            nums.append(num)

        def place_body(place, c2):
            num = nums[0]
            for which in range(1, NMAT):
                num = jnp.where(place == which, nums[which], num)
            mat = NMAT - 1 - place

            @pl.when(num >= 0)
            def _():
                for want in range(13):
                    @pl.when(num == want)
                    def _(want=want):
                        ex.step(mat, want)
            return c2
        most = jnp.maximum(jnp.maximum(nums[0], nums[1]), jnp.maximum(nums[2], nums[3]))

        @pl.when(most >= 0)
        def _():
            lax.fori_loop(0, NMAT, place_body, 0)

        @pl.when(now >= COMPUTE_SLOTS)
        def _():
            late(now)
        return carry

    lax.fori_loop(0, SLOTS, slot_body, 0)
    for item in range(NMAT * PIECES - (LANES - AHEAD), NMAT * PIECES):
        adam_flush(item)
    pltpu.make_async_remote_copy(src_ref=dh_pair, dst_ref=dh_pair, send_sem=w_send.at[0], recv_sem=w_recv.at[0], device_id=mate, device_id_type=MESH).wait()
    ex.drain()


def backward(acts, clip_norm, masters, moms, vels):
    bf16 = jnp.bfloat16
    sds = jax.ShapeDtypeStruct
    dma = pltpu.SemaphoreType.DMA
    rows = [sds((HALF, FF), F32), sds((OWN, D), F32)]
    half_w = [sds((HALF, FF), bf16), sds((OWN, D), bf16)]
    in_vmem = pl.BlockSpec(memory_space=pltpu.VMEM)
    kept = [pltpu.VMEM((NMAT, OWN, D), F32), pltpu.VMEM((BOTH, D, FF), bf16)]
    swaps = [sds((D, HALF), bf16), sds((D, OWN), bf16), sds((D, OWN), bf16)]
    outs = pl.pallas_call(
        backward_kernel,
        out_shape=half_w * 2 + rows * 4 + kept + [rows[0], sds((OCT, LANE), F32)] + swaps,
        in_specs=[HBM_ANY] * (N_ACTS - 1) + [in_vmem] + [HBM_ANY] * (N_STATE * NMAT),
        out_specs=[HBM_ANY] * (N_STATE * NMAT) + [in_vmem] * len(kept) + [HBM_ANY, in_vmem] + [HBM_ANY] * len(swaps),
        scratch_shapes=[
            pltpu.VMEM((NSET, AXES, AXES, BOTH) + HALF_SHAPE[0], F32),
            pltpu.VMEM((NSET, AXES, AXES, BOTH) + HALF_SHAPE[1], F32),
            pltpu.VMEM((NSET, AXES, AXES, BOTH) + HALF_SHAPE[2], F32),
            pltpu.VMEM((NMAT + 1, NMAT + 1, OCT, LANE), F32),
            pltpu.VMEM((OCT, LANE), F32),
            pltpu.VMEM((BOTH * D, D), bf16),
            pltpu.VMEM((BOTH * D, HALF), bf16),
            pltpu.VMEM((2, BOTH * D, TILE), bf16),
            pltpu.VMEM((2, TILE, FF), bf16),
            pltpu.VMEM((2, D, HALF), bf16),
            dma((NMAT, AXES)),
            dma((NMAT, AXES, BOTH)),
            dma((NMAT, AXES)),
            dma((NMAT, AXES, BOTH)),
            pltpu.SemaphoreType.REGULAR((NMAT, AXES)),
            pltpu.SemaphoreType.REGULAR((NMAT, AXES)),
            dma((4, 4)),
            dma((4, 4)),
            dma((2, 2)),
            dma((2, 3)),
            dma((BOTH,)),
            dma((4,)),
            dma((BOTH,)),
            dma((BOTH,)),
            dma((BOTH,)),
            dma((TILES, BOTH)),
            dma((TILES, BOTH)),
            dma((2, 6, 2)),
            dma((4, 2)),
            dma((LANES, 3)),
            dma((LANES, N_STATE)),
            dma((1,)),
            dma((1,)),
        ],
        compiler_params=pltpu.CompilerParams(collective_id=0, has_side_effects=True, vmem_limit_bytes=SCOPED_BYTES),
        name='backward_exchange',
    )(*acts, clip_norm.reshape(1, 1), *masters, *moms, *vels)
    return outs[:N_STATE * NMAT], outs[N_STATE * NMAT:N_STATE * NMAT + N_LATE - N_STATE]


RING_SLOTS = 8
READS_AHEAD = 4


def finish_kernel(*refs):
    mate_w, masters, vels = (take(refs, NMAT, which * NMAT) for which in range(N_STATE))
    moms, own_w, last_mom, norm_in = take(refs, NMAT, N_STATE * NMAT)
    outs = refs[N_STATE * NMAT + NMAT:]
    new_w, new_masters, new_moms, new_vels = (take(outs, NMAT, which * NMAT) for which in range(NMAT))
    norm_out, wide, narrow, wide_in, wide_out, narrow_in, narrow_out, direct_sem = outs[NMAT * NMAT:]
    norm_out[0, 0] = norm_in[0, 0]
    core = lax.axis_index('data')

    def block(ref, mat, stream, shift=0):
        if mat in (1, 3):
            return ref.at[pl.ds(pl.multiple_of(shift + stream * HALF, HALF), HALF), :]
        return ref.at[pl.ds(pl.multiple_of(shift, HALF), HALF), pl.ds(stream * D, D)]

    def w_block(mat, stream, side):
        return block(new_w[mat], mat, stream, side * (OWN if mat in (1, 3) else HALF))

    direct, wides, narrows = [], [], []
    for mat in range(NMAT):
        for stream in range(AXES):
            part = (mat % BOTH) * AXES + stream
            own = own_w.at[mat // BOTH, pl.ds((part % BOTH) * HALF, HALF), pl.ds((part // BOTH) * D, D)]
            direct.append((own, w_block(mat, stream, core)))
            narrows.append((block(mate_w[mat], mat, stream), w_block(mat, stream, 1 - core)))
            wides.append((block(vels[mat], mat, stream), block(new_vels[mat], mat, stream)))
            wides.append((block(masters[mat], mat, stream), block(new_masters[mat], mat, stream)))
            if mat == 0:
                wides.append((block(last_mom, mat, stream), block(new_moms[mat], mat, stream)))
            else:
                direct.append((moms.at[mat, pl.ds(stream * HALF, HALF), :], block(new_moms[mat], mat, stream)))

    def ring(items, buf, in_sem, out_sem):
        def load(idx):
            return pltpu.make_async_copy(items[idx][0], buf.at[idx % RING_SLOTS], in_sem.at[idx % RING_SLOTS])

        def store(idx):
            return pltpu.make_async_copy(buf.at[idx % RING_SLOTS], items[idx][1], out_sem.at[idx % RING_SLOTS])

        def prime():
            for idx in range(READS_AHEAD):
                load(idx).start()

        def advance(idx):
            load(idx).wait()
            store(idx).start()
            ahead = idx + READS_AHEAD
            if ahead < len(items):
                if ahead >= RING_SLOTS:
                    store(ahead - RING_SLOTS).wait()
                load(ahead).start()

        def finish():
            for idx in range(len(items) - RING_SLOTS, len(items)):
                store(idx).wait()
        return prime, advance, finish

    wide_ring = ring(wides, wide, wide_in, wide_out)
    narrow_ring = ring(narrows, narrow, narrow_in, narrow_out)
    wide_ring[0]()
    narrow_ring[0]()
    straight = [pltpu.make_async_copy(src, dst, direct_sem.at[idx]) for idx, (src, dst) in enumerate(direct)]
    for idx in range(len(wides)):
        if idx < len(straight):
            straight[idx].start()
        wide_ring[1](idx)
        if idx < len(narrows):
            narrow_ring[1](idx)
    wide_ring[2]()
    narrow_ring[2]()
    for copy in straight:
        copy.wait()


def finish(late, kept, last_mom, norm_block):
    sds = jax.ShapeDtypeStruct
    bf16 = jnp.bfloat16
    dma = pltpu.SemaphoreType.DMA
    rows = [sds((HALF, FF), F32), sds((OWN, D), F32)]
    in_vmem = pl.BlockSpec(memory_space=pltpu.VMEM)
    held = [pltpu.with_memory_space_constraint(value, pltpu.VMEM) for value in kept]
    return pl.pallas_call(
        finish_kernel,
        out_shape=[sds((D, FF), bf16), sds((FF, D), bf16)] * 2 + rows * 6 + [sds((1, 1), F32)],
        in_specs=[HBM_ANY] * (N_STATE * NMAT) + [in_vmem] * BOTH + [HBM_ANY, in_vmem],
        out_specs=[HBM_ANY] * (NMAT * NMAT) + [pl.BlockSpec(memory_space=pltpu.SMEM)],
        scratch_shapes=[
            pltpu.VMEM((RING_SLOTS, HALF, D), F32),
            pltpu.VMEM((RING_SLOTS, HALF, D), bf16),
            dma((RING_SLOTS,)),
            dma((RING_SLOTS,)),
            dma((RING_SLOTS,)),
            dma((RING_SLOTS,)),
            dma((NMAT * OCT,)),
        ],
        compiler_params=pltpu.CompilerParams(vmem_limit_bytes=SCOPED_BYTES),
        name='write_out',
    )(*late, *held, last_mom, norm_block)


def gelu_fn(values):
    return jax.nn.gelu(values, approximate=True)


def forward(act_in, w_one, w_two, w_three):
    bf16 = jnp.bfloat16
    h_one = jnp.dot(act_in, w_one, preferred_element_type=F32).astype(bf16)
    a_one = gelu_fn(h_one.astype(F32)).astype(bf16)
    y_one = jnp.dot(a_one, w_two, preferred_element_type=F32).astype(bf16)
    h_two = jnp.dot(y_one, w_three, preferred_element_type=F32).astype(bf16)
    a_two = gelu_fn(h_two.astype(F32)).astype(bf16)
    return h_one, a_one, y_one, h_two, a_two


def solution(mesh):
    row_spec = P(('rep', 'data'), None)
    shard_spec = P('data', None)
    full_spec = P()

    def per_device(act_in, grad_out, w_one, w_two, w_three, w_four, master_one, master_two, master_three, master_four, mom_one, mom_two, mom_three, mom_four, vel_one, vel_two, vel_three, vel_four, clip_norm):
        h_one, a_one, y_one, h_two, a_two = forward(act_in, w_one, w_two, w_three)
        acts = (act_in, grad_out, w_two, w_three, w_four, h_one, a_one, y_one, h_two, a_two)
        late, (grads, own_w, last_mom, norm_block) = backward(acts, clip_norm, (master_one, master_two, master_three, master_four), (mom_one, mom_two, mom_three, mom_four), (vel_one, vel_two, vel_three, vel_four))
        *new_state, grad_norm = finish(late, (grads, own_w), last_mom, norm_block)
        return tuple(new_state) + (grad_norm.reshape(()),)

    in_specs = (row_spec, row_spec, full_spec, full_spec, full_spec, full_spec) + (shard_spec,) * 12 + (full_spec,)
    out_specs = (full_spec,) * 4 + (shard_spec,) * 12 + (full_spec,)
    return jax.shard_map(per_device, mesh=mesh, in_specs=in_specs, out_specs=out_specs, check_vma=False)
```

```python
import jax
import jax.numpy as jnp
from jax import lax
from jax.experimental import pallas as pl
from jax.experimental.pallas import tpu as pltpu
from jax.sharding import PartitionSpec as P

TRAIN_STEP = 10
BETA_ONE = 0.9
BETA_TWO = 0.95
ADAM_EPS = 1e-8
NORM_EPS = 1e-6
LEARN_RATE = 0.003
STEP_SIZE = LEARN_RATE / (1.0 - BETA_ONE ** TRAIN_STEP)
VEL_GAIN = 1.0 / (1.0 - BETA_TWO ** TRAIN_STEP)
MESH = pl.DeviceIdType.MESH
NMAT = 4
F32 = jnp.float32
D = 1024
FF = 3072
HALF = 512
TILE = 256
HALF_SHAPE = ((64, D), (16, D), (8, D))
STEPS = 12
CHUNK_ROWS = (128, 32, 8)
AXES = 3
RING = 4
BOTH = 2
NSET = 2


class Torus:
    def __init__(self):
        self.rep = lax.axis_index('rep')
        self.core = lax.axis_index('data')

    def stride(self, axis):
        return 1 + 3 * lax.rem(axis, 3) + 9 * lax.div(lax.rem(axis, 3), 2)

    def pos(self, axis):
        return lax.rem(lax.div(self.rep, self.stride(axis)), 4)

    def peer(self, axis, delta):
        stride = self.stride(axis)
        pos = lax.rem(lax.div(self.rep, stride), 4)
        return {'rep': self.rep + (lax.rem(pos + delta + 4, 4) - pos) * stride, 'data': self.core}


class Exchange:
    def __init__(self, tor, grads, slots, norm_buf, rs_send, rs_recv, ag_send, ag_recv, free_sem, slot_sem, nm_send, nm_recv):
        self.free_sem, self.slot_sem = free_sem, slot_sem
        self.tor, self.grads, self.slots = tor, grads, slots
        self.pos = [tor.pos(axis) for axis in range(AXES)]
        self.base = []
        for stream in range(AXES):
            base = stream * HALF
            for level in range(AXES):
                self.base.append(base)
                base = base + self.pos[(stream + level) % AXES] * CHUNK_ROWS[level]
        self.norm_buf = norm_buf
        self.rs_send, self.rs_recv, self.ag_send, self.ag_recv = rs_send, rs_recv, ag_send, ag_recv
        self.nm_send, self.nm_recv = nm_send, nm_recv

    def neighbour(self, stream, level, side):
        axis = (stream + level) % AXES
        pos = self.pos[axis]
        return {'rep': self.tor.rep + (lax.rem(pos + 1 + BOTH * side, RING) - pos) * RING ** axis, 'data': self.tor.core}

    def region(self, mat, stream, level, delta, half):
        rows = CHUNK_ROWS[level]
        row = self.base[stream * AXES + level] + lax.rem(self.pos[(stream + level) % AXES] + delta, RING) * rows
        row = pl.multiple_of(row + half * (rows // BOTH), rows // BOTH)
        return self.grads.at[mat, pl.ds(row, rows // BOTH), :]

    def chunk(self, mat, stream, delta):
        rows = CHUNK_ROWS[BOTH]
        row = self.base[stream * AXES + BOTH] + lax.rem(self.pos[(stream + BOTH) % AXES] + delta, RING) * rows
        return self.grads.at[mat, pl.ds(pl.multiple_of(row, rows), rows), :]

    def ringmate(self, stream, delta):
        axis = (stream + BOTH) % AXES
        pos = self.pos[axis]
        return {'rep': self.tor.rep + (lax.rem(pos + delta, RING) - pos) * RING ** axis, 'data': self.tor.core}

    def far_copy(self, mat, stream, delta, gather):
        src = self.chunk(mat, stream, 0 if gather else delta)
        dst = src if gather else self.slots[BOTH].at[lax.rem(mat, NSET), stream, delta - 1]
        send, recv = (self.ag_send, self.ag_recv) if gather else (self.rs_send, self.rs_recv)
        return pltpu.make_async_remote_copy(src_ref=src, dst_ref=dst, send_sem=send.at[mat, BOTH], recv_sem=recv.at[mat, BOTH, 0], device_id=self.ringmate(stream, delta), device_id_type=MESH)

    def ringmates(self, body):
        for stream in range(AXES):
            def one(delta, carry, stream=stream):
                body(stream, delta)
                return carry
            lax.fori_loop(1, RING, one, 0)

    def rs_copy(self, mat, stream, level, msg, side):
        near = 1 + BOTH * side
        if isinstance(msg, int):
            delta, half = ((BOTH, side), (near, 1 - side), (near, side))[msg]
        else:
            delta, half = BOTH + msg * (near - BOTH), side + msg * (1 - BOTH * side)
        return pltpu.make_async_remote_copy(
            src_ref=self.region(mat, stream, level, delta, half),
            dst_ref=self.slots[level].at[lax.rem(mat, NSET), stream, msg, side],
            send_sem=self.rs_send.at[mat, level],
            recv_sem=self.rs_recv.at[mat, level, msg - msg // BOTH if isinstance(msg, int) else msg],
            device_id=self.neighbour(stream, level, side), device_id_type=MESH)

    def ag_copy(self, mat, stream, level, msg, side):
        if isinstance(msg, int):
            delta, half = ((0, side), (0, 1 - side), (RING - 1 - BOTH * side, side))[msg]
        else:
            delta, half = 0, side + msg * (1 - BOTH * side)
        ref = self.region(mat, stream, level, delta, half)
        return pltpu.make_async_remote_copy(
            src_ref=ref, dst_ref=ref,
            send_sem=self.ag_send.at[mat, level],
            recv_sem=self.ag_recv.at[mat, level, msg],
            device_id=self.neighbour(stream, level, side), device_id_type=MESH)

    def pairs(self, body, msgs=1):
        for stream in range(AXES):
            def one(idx, carry, stream=stream):
                body(stream, lax.rem(idx, BOTH), lax.div(idx, BOTH))
                return carry
            lax.fori_loop(0, BOTH * msgs, one, 0)

    def bulk(self, mat, level, late, gather):
        send, recv = (self.ag_send, self.ag_recv) if gather else (self.rs_send, self.rs_recv)
        kinds = AXES if late is None else 1 if gather else 1 + late
        count = AXES * AXES if level == BOTH else AXES * BOTH * kinds
        rows = count * HALF_SHAPE[level][0] * HALF_SHAPE[level][1] // D
        ref = self.grads.at[mat, pl.ds(0, rows), :]
        copy = pltpu.make_async_remote_copy(src_ref=ref, dst_ref=ref, send_sem=send.at[mat, level], recv_sem=recv.at[mat, level, late or 0], device_id=self.neighbour(0, level, 0), device_id_type=MESH)
        if late is None:
            copy.wait_send()
        else:
            copy.wait_recv()

    def rs_first(self, mat, level):
        @pl.when(mat < NMAT - NSET)
        def _():
            pl.semaphore_wait(self.slot_sem.at[mat, level], AXES * BOTH)
        self.pairs(lambda stream, side, msg: self.rs_copy(mat, stream, level, msg, side).start(), BOTH)

    def rs_mid(self, mat, level):
        self.bulk(mat, level, 0, False)

        def body(stream, side, _):
            ref = self.region(mat, stream, level, 1 + BOTH * side, side)
            ref[...] = ref[...] + self.slots[level][lax.rem(mat, NSET), stream, 0, side]
            self.rs_copy(mat, stream, level, BOTH, side).start()
        self.pairs(body)

    def rs_last(self, mat, level):
        self.bulk(mat, level, 1, False)
        self.bulk(mat, level, None, False)

        def body(stream, half, _):
            ref = self.region(mat, stream, level, 0, half)
            held = self.slots[level]
            total = ref[...] + held[lax.rem(mat, NSET), stream, 2, half] + held[lax.rem(mat, NSET), stream, 1, 1 - half]
            ref[...] = total
        self.pairs(body)

        def tell(stream, side, _):
            peer = self.neighbour(stream, level, side)
            pl.semaphore_signal(self.free_sem.at[mat, level], inc=1, device_id=peer, device_id_type=MESH)

            @pl.when(mat >= NSET)
            def _():
                pl.semaphore_signal(self.slot_sem.at[mat - NSET, level], inc=1, device_id=peer, device_id_type=MESH)
        self.pairs(tell)

    def ag_first(self, mat, level):
        pl.semaphore_wait(self.free_sem.at[mat, level], AXES * BOTH)
        self.pairs(lambda stream, side, msg: self.ag_copy(mat, stream, level, msg, side).start(), BOTH)

    def ag_mid(self, mat, level):
        self.bulk(mat, level, 0, True)
        self.pairs(lambda stream, side, _: self.ag_copy(mat, stream, level, BOTH, side).start())

    def far_first(self, mat):
        @pl.when(mat < NMAT - NSET)
        def _():
            pl.semaphore_wait(self.slot_sem.at[mat, BOTH], AXES * AXES)
        self.ringmates(lambda stream, delta: self.far_copy(mat, stream, delta, False).start())

    def far_last(self, mat):
        self.bulk(mat, BOTH, 0, False)
        self.bulk(mat, BOTH, None, False)
        held = self.slots[BOTH]
        for stream in range(AXES):
            ref = self.chunk(mat, stream, 0)
            total = (ref[...] + held[lax.rem(mat, NSET), stream, 0] + held[lax.rem(mat, NSET), stream, 1] + held[lax.rem(mat, NSET), stream, 2]) * (1.0 / LANE)
            square = total * total
            self.norm_buf[4, 0] = self.norm_buf[4, 0] + sum(square[:, col * LANE:(col + 1) * LANE] for col in range(OCT))
            ref[...] = total

        def tell(stream, delta):
            peer = self.ringmate(stream, delta)
            pl.semaphore_signal(self.free_sem.at[mat, BOTH], inc=1, device_id=peer, device_id_type=MESH)

            @pl.when(mat >= NSET)
            def _():
                pl.semaphore_signal(self.slot_sem.at[mat - NSET, BOTH], inc=1, device_id=peer, device_id_type=MESH)
        self.ringmates(tell)

    def far_gather(self, mat):
        pl.semaphore_wait(self.free_sem.at[mat, BOTH], AXES * AXES)
        self.ringmates(lambda stream, delta: self.far_copy(mat, stream, delta, True).start())

    def step(self, mat, num):
        if num == 0:
            self.rs_first(mat, 0)
        elif num in (1, 3):
            self.rs_mid(mat, num // 2)
        elif num == 2:
            self.rs_last(mat, 0)
            self.rs_first(mat, 1)
        elif num == 4:
            self.rs_last(mat, 1)
            self.far_first(mat)
        elif num == 5:
            self.far_last(mat)
            self.far_gather(mat)
        elif num == 6:
            self.bulk(mat, BOTH, 0, True)
            self.ag_first(mat, 1)
        elif num in (7, 9):
            self.ag_mid(mat, (9 - num) // 2)
        elif num == 8:
            self.bulk(mat, 1, 1, True)
            self.bulk(mat, 1, BOTH, True)
            self.ag_first(mat, 0)
        elif num == 10:
            self.bulk(mat, 0, 1, True)
        else:
            self.bulk(mat, 0, BOTH, True)
            for level in range(AXES):
                self.bulk(mat, level, None, True)

    def norm_copy(self, stage, delta):
        tor = self.tor
        if stage < 3:
            mine, dev = tor.pos(stage), tor.peer(stage, delta)
        else:
            mine, dev = tor.core, {'data': 1 - tor.core}
        return pltpu.make_async_remote_copy(
            src_ref=self.norm_buf.at[4, stage], dst_ref=self.norm_buf.at[stage, mine],
            send_sem=self.nm_send.at[stage, delta], recv_sem=self.nm_recv.at[stage, delta],
            device_id=dev, device_id_type=MESH)

    def deltas(self, stage):
        return (1, 2, 3) if stage < AXES else (1,)

    def norm_start(self, stage):
        for delta in (self.deltas(stage)):
            self.norm_copy(stage, delta).start()
        mine = self.tor.pos(stage) if stage < 3 else self.tor.core
        self.norm_buf[stage, mine] = self.norm_buf[4, stage]

    def norm_finish(self, stage):
        for delta in (self.deltas(stage)):
            self.norm_copy(stage, delta).wait_recv()
        total = self.norm_buf[stage, 0] + self.norm_buf[stage, 1]
        if stage < 3:
            total = total + self.norm_buf[stage, 2] + self.norm_buf[stage, 3]
            self.norm_buf[4, stage + 1] = total
        else:
            self.norm_buf[4, 4] = total

    def drain(self):
        for stage in range(4):
            for delta in (self.deltas(stage)):
                self.norm_copy(stage, delta).wait_send()

    def greet(self):
        tor = self.tor
        barrier = pltpu.get_barrier_semaphore()
        for axis in range(AXES):
            for delta in (1, 2, 3):
                pl.semaphore_signal(barrier, inc=1, device_id=tor.peer(axis, delta), device_id_type=MESH)
        pl.semaphore_signal(barrier, inc=1, device_id={'data': 1 - tor.core}, device_id_type=MESH)
        return barrier


SUB = 64
OCT = 8
LANE = 128
OWN = 1536
TILES = 6
HBM_ANY = pl.BlockSpec(memory_space=pl.ANY)
ROWS_ROWS = (((0,), (0,)), ((), ()))
COLS_COLS = (((1,), (1,)), ((), ()))
COMPUTE_SLOTS = 7 * TILES + RING
FIRST_SWAP = 2
STEP_SLOTS = (
    (11, 15, 20, 22, 26, 28, 30, 32, 34, 51, 54, 58),
    (23, 26, 29, 32, 46, 48, 50, 52, 55, 60, 65, 66),
    (33, 38, 46, 47, 49, 51, 54, 57, 63, 71, 74, 76),
    (45, 46, 48, 49, 50, 52, 64, 75, 78, 83, 88, 89),
)
NORM_SLOTS = (52, 53, 54, 55, 56)
ADAM_RUNS = ((58, 6, 0), (65, 10, 6), (76, 16, 16))
ADAM_READY = 49
LANES = 12
AHEAD = 8
PER_SLOT = 3
PIECES = 24
SLOTS = 92
GELU_A = 0.7978845608028654
GELU_B = 0.044715


def gelu_slope(hidden):
    square = hidden * hidden
    tanh = jnp.tanh(hidden * (GELU_A + GELU_A * GELU_B * square))
    return 0.5 * (1.0 + tanh) + (0.5 * hidden) * (1.0 - tanh * tanh) * (GELU_A + 3.0 * GELU_A * GELU_B * square)


N_ACTS = 11
N_STATE = 3
N_LATE = 7
LAST = (NMAT - 1) * PIECES
SCOPED_BYTES = 67043328 - (NMAT * OWN * D * 4 + 2 * D * FF * 2)


def take(refs, count, start=0):
    return refs[start:start + count]


def backward_kernel(*refs):
    x_in, dy_in, w_two, w_three, w_four, h_one, a_one, y_one, h_two, a_two, clip_ref = take(refs, N_ACTS)
    masters, moms, vels = (take(refs, NMAT, N_ACTS + which * NMAT) for which in range(N_STATE))
    outs = refs[N_ACTS + N_STATE * NMAT:]
    mate_w, new_masters, new_vels = (take(outs, NMAT, which * NMAT) for which in range(N_STATE))
    grads, dh_pair, last_mom, norm_ref, x_peer, a_one_peer, a_two_peer = take(outs, N_LATE, N_STATE * NMAT)
    (slot_big, slot_mid, slot_low, norm_buf, scale_ref, dy_pair, y_pair, a_tile, w_tile, h_tile,
     rs_send, rs_recv, ag_send, ag_recv, free_sem, slot_sem, nm_send, nm_recv,
     a_tile_sem, w_tile_sem, h_tile_sem, load_sem, dyx_sem, yx_sem, xx_sem, a_one_sem, a_two_sem, dh_sem, dyp_sem,
     in_sem, out_sem, w_send, w_recv) = outs[N_STATE * NMAT + N_LATE:]
    dh_own, dh_peer = dh_pair.at[0], dh_pair.at[1]
    tor = Torus()
    ex = Exchange(tor, grads, (slot_big, slot_mid, slot_low), norm_buf, rs_send, rs_recv, ag_send, ag_recv, free_sem, slot_sem, nm_send, nm_recv)
    core = tor.core
    other = 1 - core
    mate = {'data': other}

    def send(src, dst, sem):
        return pltpu.make_async_remote_copy(src_ref=src, dst_ref=dst, send_sem=sem.at[0], recv_sem=sem.at[1], device_id=mate, device_id_type=MESH)

    def columns(start, size):
        return pl.ds(pl.multiple_of(start, size), size)

    def piece_rows(index, base=0):
        return pl.ds(pl.multiple_of(base + index * SUB, SUB), SUB)

    dy_swap = send(dy_in, dy_pair.at[pl.ds(D, D), :], dyx_sem)
    y_swap = send(y_one.at[:, columns(other * HALF, HALF)], y_pair.at[pl.ds(D, D), :], yx_sem)
    x_swap = send(x_in.at[:, columns(other * HALF, HALF)], x_peer, xx_sem)

    def a_swap(layer, tile):
        src, dst, sem = ((a_one, a_one_peer, a_one_sem), (a_two, a_two_peer, a_two_sem))[layer]
        return send(src.at[:, columns(other * OWN + tile * TILE, TILE)], dst.at[:, columns(tile * TILE, TILE)], sem.at[tile])

    def dh_swap(layer, tile):
        return send(dh_own.at[:, columns(tile * HALF, HALF)], dh_peer.at[:, columns(tile * HALF, HALF)], dh_sem.at[layer, tile])

    def dyp_swap(tile):
        return send(dy_pair.at[pl.ds(0, D), columns(tile * TILE, TILE)], dy_pair.at[pl.ds(D, D), columns(tile * TILE, TILE)], dyp_sem.at[tile])

    def a_load(layer, tile, part):
        slot = lax.rem(tile, BOTH)
        if part == 0:
            src = (a_one, a_two)[layer].at[:, columns(core * OWN + tile * TILE, TILE)]
        else:
            src = (a_one_peer, a_two_peer)[layer].at[:, columns(tile * TILE, TILE)]
        return pltpu.make_async_copy(src, a_tile.at[slot, pl.ds(part * D, D), :], a_tile_sem.at[slot, part])

    def w_load(layer, tile):
        slot = lax.rem(tile, BOTH)
        src = (w_two, w_four)[layer].at[pl.ds(pl.multiple_of(tile * HALF, HALF), HALF), :]
        return [pltpu.make_async_copy(src.at[pl.ds(part * TILE, TILE), :], w_tile.at[slot, :, pl.ds(part * D, D)], w_tile_sem.at[slot, part]) for part in range(2)]

    def w_three_load(tile):
        slot = lax.rem(tile, BOTH)
        return [pltpu.make_async_copy(w_three.at[pl.ds(pl.multiple_of(tile * TILE, TILE), TILE), :], w_tile.at[slot], w_tile_sem.at[slot, 0])]

    def h_load(layer, tile):
        slot = lax.rem(tile, BOTH)
        return pltpu.make_async_copy((h_one, h_two)[layer].at[:, columns(tile * HALF, HALF)], h_tile.at[slot], h_tile_sem.at[slot])

    def start_all(copies):
        for copy in copies:
            copy.start()

    def wait_all(copies):
        for copy in copies:
            copy.wait()

    dy_load = pltpu.make_async_copy(dy_in, dy_pair.at[pl.ds(0, D), :], load_sem.at[0])
    y_load = pltpu.make_async_copy(y_one.at[:, columns(core * HALF, HALF)], y_pair.at[pl.ds(0, D), :], load_sem.at[1])
    x_load = pltpu.make_async_copy(x_in.at[:, columns(core * HALF, HALF)], y_pair.at[pl.ds(0, D), :], load_sem.at[2])
    x_peer_load = pltpu.make_async_copy(x_peer, y_pair.at[pl.ds(D, D), :], load_sem.at[3])

    dy_load.start()
    start_all(w_load(1, 0))
    h_load(1, 0).start()
    a_load(1, 0, 0).start()
    y_load.start()
    barrier = ex.greet()
    norm_buf[4, 0] = jnp.zeros((OCT, LANE), F32)
    dy_load.wait()

    def first_swaps():
        pl.semaphore_wait(barrier, 10)
        dy_swap.start()
        for layer in (1, 0):
            def swap_one(tile, carry, layer=layer):
                a_swap(layer, tile).start()
                return carry
            lax.fori_loop(0, TILES, swap_one, 0)
            if layer == 1:
                y_swap.start()
        x_swap.start()

    def dh_slot(layer, tile):
        slot = lax.rem(tile, BOTH)

        @pl.when(tile < TILES - 1)
        def _():
            start_all(w_load(layer, tile + 1))
            h_load(layer, tile + 1).start()

        if layer == 1:
            @pl.when(tile == TILES - 1)
            def _():
                start_all(w_three_load(0))
        wait_all(w_load(layer, tile))
        h_load(layer, tile).wait()
        def part_body(part, carry):
            rows = pl.ds(pl.multiple_of(part * HALF, HALF), HALF)
            for half in range(2):
                acc = lax.dot_general(dy_pair[rows, :], w_tile[slot, :, half * D:(half + 1) * D], COLS_COLS, preferred_element_type=F32)
                slope = gelu_slope(h_tile[slot, rows, half * TILE:(half + 1) * TILE].astype(F32))
                dh_own[rows, columns(tile * HALF + half * TILE, TILE)] = (slope * acc.astype(jnp.bfloat16).astype(F32)).astype(jnp.bfloat16)
            return carry
        lax.fori_loop(0, BOTH, part_body, 0)
        dh_swap(layer, tile).start()

    def row_slot(tile):
        slot = lax.rem(tile, BOTH)

        @pl.when(tile == 0)
        def _():
            for part in range(RING):
                dyp_swap(part).wait()
            a_swap(0, tile).wait()
            a_load(0, tile, 1).start()

        @pl.when(tile < TILES - 1)
        def _():
            a_load(0, tile + 1, 0).start()
            a_swap(0, tile + 1).wait()
            a_load(0, tile + 1, 1).start()
        a_load(0, tile, 0).wait()
        a_load(0, tile, 1).wait()
        grads[1, pl.ds(pl.multiple_of(tile * TILE, TILE), TILE), :] = lax.dot_general(a_tile[slot], dy_pair[...], ROWS_ROWS, preferred_element_type=F32)

    def half_slot(part, tile):
        slot = lax.rem(tile, BOTH)

        @pl.when(tile == 0)
        def _():
            if part == 1:
                dy_swap.wait()
                y_swap.wait_send()
                a_swap(1, tile).wait()
                a_load(1, tile, part).start()

        @pl.when(tile < TILES - 1)
        def _():
            if part == 1:
                a_swap(1, tile + 1).wait()
            a_load(1, tile + 1, part).start()
        a_load(1, tile, part).wait()
        rows = pl.ds(pl.multiple_of(tile * TILE, TILE), TILE)
        mine = slice(part * D, part * D + D)
        total = lax.dot_general(a_tile[slot, mine, :], dy_pair[mine, :], ROWS_ROWS, preferred_element_type=F32)
        grads[AXES, rows, :] = total if part == 0 else grads[AXES, rows, :] + total

    def column_slot(layer, tile):
        @pl.when(tile == 0)
        def _():
            if layer == 1:
                y_load.wait()
                y_swap.wait_recv()
            else:
                x_load.wait()
                x_peer_load.wait()
        dh_swap(layer, tile).wait()
        cols = columns(tile * HALF, HALF)

        total = lax.dot_general(y_pair[0:D, :], dh_own[:, cols], ROWS_ROWS, preferred_element_type=F32)
        total = total + lax.dot_general(y_pair[D:BOTH * D, :], dh_peer[:, cols], ROWS_ROWS, preferred_element_type=F32)
        rows = pl.ds(pl.multiple_of(lax.div(tile, BOTH) * HALF, HALF), HALF)
        grads[2 * layer, rows, columns(lax.rem(tile, BOTH) * HALF, HALF)] = total

    def dy_slot(tile):
        slot = lax.rem(tile, BOTH)

        @pl.when(tile < 3)
        def _():
            start_all(w_three_load(tile + 1))

        @pl.when(tile == 3)
        def _():
            start_all(w_load(0, 0))
            h_load(0, 0).start()
            a_load(0, 0, 0).start()
            x_load.start()
            x_swap.wait()
            x_peer_load.start()
        wait_all(w_three_load(tile))

        def part_body(part, carry):
            rows = pl.ds(pl.multiple_of(part * HALF, HALF), HALF)
            acc = lax.dot_general(dh_own[rows, :], w_tile[slot], COLS_COLS, preferred_element_type=F32)
            dy_pair[rows, columns(tile * TILE, TILE)] = acc.astype(jnp.bfloat16)
            return carry
        lax.fori_loop(0, BOTH, part_body, 0)
        dyp_swap(tile).start()

    def lane_tile(item, which):
        lane = lax.rem(item, LANES)
        return slot_big.at[lax.div(lane, 6), lax.rem(lax.div(lane, 2), 3), which, lax.rem(lane, 2)]

    def w_stage(mat, piece):
        part = lax.rem(mat, BOTH) * AXES + lax.div(piece, OCT)
        return dh_pair.at[lax.div(mat, BOTH), piece_rows(lax.rem(piece, OCT), lax.rem(part, BOTH) * HALF), columns(lax.div(part, BOTH) * D, D)]

    def state_view(ref, mat, piece):
        if mat in (1, 3):
            return ref.at[piece_rows(piece), :]
        return ref.at[piece_rows(lax.rem(piece, OCT)), columns(lax.div(piece, OCT) * D, D)]

    def state_load(item, which, mat, piece):
        return pltpu.make_async_copy(state_view((moms, vels, masters)[which][mat], mat, piece), lane_tile(item, which), in_sem.at[lax.rem(item, LANES), which])

    def state_store(item, which, mat, piece):
        target = last_mom if which == 0 else (new_vels, new_masters)[which - 1][mat]
        return pltpu.make_async_copy(lane_tile(item, which), state_view(target, mat, piece), out_sem.at[lax.rem(item, LANES), which])

    def w_swap(item, mat, piece):
        return pltpu.make_async_remote_copy(src_ref=w_stage(mat, piece), dst_ref=state_view(mate_w[mat], mat, piece), send_sem=w_send.at[0], recv_sem=w_recv.at[0], device_id=mate, device_id_type=MESH)

    def piece_of(item):
        idx = lax.rem(item, PIECES)
        group = lax.div(idx, TILES)
        stream = lax.div(lax.rem(idx, TILES), BOTH)
        odd = lax.rem(idx, BOTH)
        delta = jnp.where(group == 0, 0, jnp.where(group == AXES, BOTH, AXES - BOTH * odd))
        half = jnp.where(group == BOTH, 1 - odd, odd)
        pos = jnp.where(stream == 0, ex.pos[0], jnp.where(stream == 1, ex.pos[1], ex.pos[2]))
        return stream * OCT + lax.rem(pos + delta, RING) * BOTH + half

    def for_mat(item, body):
        place = lax.div(item, PIECES)
        piece = piece_of(item)
        for which in range(NMAT):
            @pl.when(place == which)
            def _(which=which):
                body(NMAT - 1 - which, piece)

    def adam_fetch(item):
        def body(mat, piece):
            for which in range(N_STATE):
                state_load(item, which, mat, piece).start()
        for_mat(item, body)

    def adam_flush(item):
        for which in (1, 2):
            state_store(item, which, 1, 0).wait()

        @pl.when(item >= LAST)
        def _():
            state_store(item, 0, 0, 0).wait()

    def adam_item(item):
        @pl.when(item >= LANES - AHEAD)
        def _():
            adam_flush(item - (LANES - AHEAD))

        @pl.when(item < NMAT * PIECES - AHEAD)
        def _():
            adam_fetch(item + AHEAD)
        for which in range(N_STATE):
            state_load(item, which, 1, 0).wait()
        mom, vel, master = (lane_tile(item, which) for which in range(N_STATE))
        mat, piece = NMAT - 1 - lax.div(item, PIECES), piece_of(item)
        scaled = scale_ref[0:1, 0:1] * grads[mat, piece_rows(piece), :]
        mom_new = BETA_ONE * mom[...] + (1.0 - BETA_ONE) * scaled
        vel_new = BETA_TWO * vel[...] + (1.0 - BETA_TWO) * jnp.square(scaled)
        master_new = master[...] - STEP_SIZE * mom_new / (jnp.sqrt(vel_new * VEL_GAIN) + ADAM_EPS)
        vel[...] = vel_new
        master[...] = master_new

        mom[...] = mom_new
        w_stage(mat, piece)[...] = master_new.astype(jnp.bfloat16)

        @pl.when(item < LAST)
        def _():
            grads[mat, piece_rows(piece), :] = mom[...]

        def body(mat, piece):
            for which in range(N_STATE):
                if which > 0 or mat == 0:
                    state_store(item, which, mat, piece).start()
            w_swap(item, mat, piece).start()
        for_mat(item, body)

    def set_scale():
        total = jnp.sum(jnp.sum(norm_buf[NMAT, NMAT], axis=0, keepdims=True), axis=1, keepdims=True)
        norm = jnp.sqrt(total)
        norm_ref[...] = jnp.broadcast_to(norm, norm_ref.shape)
        scale_ref[...] = jnp.broadcast_to(jnp.minimum(1.0, clip_ref[...] / (norm + NORM_EPS)), scale_ref.shape)

    def during(first, last, now, body):
        @pl.when((now >= first) & (now < last))
        def _():
            body()

    def compute(now):
        at = 0
        for count, body in ((TILES, lambda tile: half_slot(0, tile)), (TILES, lambda tile: half_slot(1, tile)), (TILES, lambda tile: dh_slot(1, tile)), (TILES, lambda tile: column_slot(1, tile)),
                            (RING, dy_slot), (TILES, row_slot), (TILES, lambda tile: dh_slot(0, tile)), (TILES, lambda tile: column_slot(0, tile))):
            during(at, at + count, now, lambda body=body, at=at: body(now - at))
            at = at + count

    def late(now):
        for stage in range(NMAT + 1):
            @pl.when(now == NORM_SLOTS[stage])
            def _(stage=stage):
                if stage > 0:
                    ex.norm_finish(stage - 1)
                if stage < NMAT:
                    ex.norm_start(stage)
                else:
                    set_scale()

        @pl.when(now == ADAM_READY)
        def _():
            for item in range(AHEAD):
                adam_fetch(item)

        first = 0
        active = 0
        for start, length, chunk in ADAM_RUNS:
            inside = (now >= start) & (now < start + length)
            first = jnp.where(inside, (now - start + chunk) * PER_SLOT, first)
            active = jnp.where(inside, 1, active)

        @pl.when(active == 1)
        def _():
            def adam_body(idx, carry):
                adam_item(first + idx)
                return carry
            lax.fori_loop(0, PER_SLOT, adam_body, 0)

    def slot_body(now, carry):
        @pl.when(now == FIRST_SWAP)
        def _():
            first_swaps()

        @pl.when(now < COMPUTE_SLOTS)
        def _():
            compute(now)

        nums = []
        for which in range(NMAT):
            num = -1
            for order, at in enumerate(STEP_SLOTS[which]):
                num = jnp.where(now == at, order, num)
            nums.append(num)

        def place_body(place, c2):
            num = nums[0]
            for which in range(1, NMAT):
                num = jnp.where(place == which, nums[which], num)
            mat = NMAT - 1 - place

            @pl.when(num >= 0)
            def _():
                for want in range(STEPS):
                    @pl.when(num == want)
                    def _(want=want):
                        ex.step(mat, want)
            return c2
        most = jnp.maximum(jnp.maximum(nums[0], nums[1]), jnp.maximum(nums[2], nums[3]))

        @pl.when(most >= 0)
        def _():
            lax.fori_loop(0, NMAT, place_body, 0)

        @pl.when(now >= COMPUTE_SLOTS)
        def _():
            late(now)
        return carry

    lax.fori_loop(0, SLOTS, slot_body, 0)
    for item in range(NMAT * PIECES - (LANES - AHEAD), NMAT * PIECES):
        adam_flush(item)
    pltpu.make_async_remote_copy(src_ref=dh_pair, dst_ref=dh_pair, send_sem=w_send.at[0], recv_sem=w_recv.at[0], device_id=mate, device_id_type=MESH).wait()
    ex.drain()


def backward(acts, clip_norm, masters, moms, vels):
    bf16 = jnp.bfloat16
    sds = jax.ShapeDtypeStruct
    dma = pltpu.SemaphoreType.DMA
    rows = [sds((HALF, FF), F32), sds((OWN, D), F32)]
    half_w = [sds((HALF, FF), bf16), sds((OWN, D), bf16)]
    in_vmem = pl.BlockSpec(memory_space=pltpu.VMEM)
    kept = [pltpu.VMEM((NMAT, OWN, D), F32), pltpu.VMEM((BOTH, D, FF), bf16)]
    swaps = [sds((D, HALF), bf16), sds((D, OWN), bf16), sds((D, OWN), bf16)]
    outs = pl.pallas_call(
        backward_kernel,
        out_shape=half_w * 2 + rows * 4 + kept + [rows[0], sds((OCT, LANE), F32)] + swaps,
        in_specs=[HBM_ANY] * (N_ACTS - 1) + [in_vmem] + [HBM_ANY] * (N_STATE * NMAT),
        out_specs=[HBM_ANY] * (N_STATE * NMAT) + [in_vmem] * len(kept) + [HBM_ANY, in_vmem] + [HBM_ANY] * len(swaps),
        scratch_shapes=[
            pltpu.VMEM((NSET, AXES, AXES, BOTH) + HALF_SHAPE[0], F32),
            pltpu.VMEM((NSET, AXES, AXES, BOTH) + HALF_SHAPE[1], F32),
            pltpu.VMEM((NSET, AXES, AXES) + HALF_SHAPE[2], F32),
            pltpu.VMEM((NMAT + 1, NMAT + 1, OCT, LANE), F32),
            pltpu.VMEM((OCT, LANE), F32),
            pltpu.VMEM((BOTH * D, D), bf16),
            pltpu.VMEM((BOTH * D, HALF), bf16),
            pltpu.VMEM((2, BOTH * D, TILE), bf16),
            pltpu.VMEM((2, TILE, FF), bf16),
            pltpu.VMEM((2, D, HALF), bf16),
            dma((NMAT, AXES)),
            dma((NMAT, AXES, BOTH)),
            dma((NMAT, AXES)),
            dma((NMAT, AXES, AXES)),
            pltpu.SemaphoreType.REGULAR((NMAT, AXES)),
            pltpu.SemaphoreType.REGULAR((NMAT, AXES)),
            dma((4, 4)),
            dma((4, 4)),
            dma((2, 2)),
            dma((2, 3)),
            dma((BOTH,)),
            dma((4,)),
            dma((BOTH,)),
            dma((BOTH,)),
            dma((BOTH,)),
            dma((TILES, BOTH)),
            dma((TILES, BOTH)),
            dma((2, 6, 2)),
            dma((4, 2)),
            dma((LANES, 3)),
            dma((LANES, N_STATE)),
            dma((1,)),
            dma((1,)),
        ],
        compiler_params=pltpu.CompilerParams(collective_id=0, has_side_effects=True, vmem_limit_bytes=SCOPED_BYTES),
        name='backward_exchange',
    )(*acts, clip_norm.reshape(1, 1), *masters, *moms, *vels)
    return outs[:N_STATE * NMAT], outs[N_STATE * NMAT:N_STATE * NMAT + N_LATE - N_STATE]


RING_SLOTS = 8
READS_AHEAD = 4


def finish_kernel(*refs):
    mate_w, masters, vels = (take(refs, NMAT, which * NMAT) for which in range(N_STATE))
    moms, own_w, last_mom, norm_in = take(refs, NMAT, N_STATE * NMAT)
    outs = refs[N_STATE * NMAT + NMAT:]
    new_w, new_masters, new_moms, new_vels = (take(outs, NMAT, which * NMAT) for which in range(NMAT))
    norm_out, wide, narrow, wide_in, wide_out, narrow_in, narrow_out, direct_sem = outs[NMAT * NMAT:]
    norm_out[0, 0] = norm_in[0, 0]
    core = lax.axis_index('data')

    def block(ref, mat, stream, shift=0):
        if mat in (1, 3):
            return ref.at[pl.ds(pl.multiple_of(shift + stream * HALF, HALF), HALF), :]
        return ref.at[pl.ds(pl.multiple_of(shift, HALF), HALF), pl.ds(stream * D, D)]

    def w_block(mat, stream, side):
        return block(new_w[mat], mat, stream, side * (OWN if mat in (1, 3) else HALF))

    direct, wides, narrows = [], [], []
    for mat in range(NMAT):
        for stream in range(AXES):
            part = (mat % BOTH) * AXES + stream
            own = own_w.at[mat // BOTH, pl.ds((part % BOTH) * HALF, HALF), pl.ds((part // BOTH) * D, D)]
            direct.append((own, w_block(mat, stream, core)))
            narrows.append((block(mate_w[mat], mat, stream), w_block(mat, stream, 1 - core)))
            wides.append((block(vels[mat], mat, stream), block(new_vels[mat], mat, stream)))
            wides.append((block(masters[mat], mat, stream), block(new_masters[mat], mat, stream)))
            if mat == 0:
                wides.append((block(last_mom, mat, stream), block(new_moms[mat], mat, stream)))
            else:
                direct.append((moms.at[mat, pl.ds(stream * HALF, HALF), :], block(new_moms[mat], mat, stream)))

    def ring(items, buf, in_sem, out_sem):
        def load(idx):
            return pltpu.make_async_copy(items[idx][0], buf.at[idx % RING_SLOTS], in_sem.at[idx % RING_SLOTS])

        def store(idx):
            return pltpu.make_async_copy(buf.at[idx % RING_SLOTS], items[idx][1], out_sem.at[idx % RING_SLOTS])

        def prime():
            for idx in range(READS_AHEAD):
                load(idx).start()

        def advance(idx):
            load(idx).wait()
            store(idx).start()
            ahead = idx + READS_AHEAD
            if ahead < len(items):
                if ahead >= RING_SLOTS:
                    store(ahead - RING_SLOTS).wait()
                load(ahead).start()

        def finish():
            for idx in range(len(items) - RING_SLOTS, len(items)):
                store(idx).wait()
        return prime, advance, finish

    wide_ring = ring(wides, wide, wide_in, wide_out)
    narrow_ring = ring(narrows, narrow, narrow_in, narrow_out)
    wide_ring[0]()
    narrow_ring[0]()
    straight = [pltpu.make_async_copy(src, dst, direct_sem.at[idx]) for idx, (src, dst) in enumerate(direct)]
    for idx in range(len(wides)):
        if idx < len(straight):
            straight[idx].start()
        wide_ring[1](idx)
        if idx < len(narrows):
            narrow_ring[1](idx)
    wide_ring[2]()
    narrow_ring[2]()
    for copy in straight:
        copy.wait()


def finish(late, kept, last_mom, norm_block):
    sds = jax.ShapeDtypeStruct
    bf16 = jnp.bfloat16
    dma = pltpu.SemaphoreType.DMA
    rows = [sds((HALF, FF), F32), sds((OWN, D), F32)]
    in_vmem = pl.BlockSpec(memory_space=pltpu.VMEM)
    held = [pltpu.with_memory_space_constraint(value, pltpu.VMEM) for value in kept]
    return pl.pallas_call(
        finish_kernel,
        out_shape=[sds((D, FF), bf16), sds((FF, D), bf16)] * 2 + rows * 6 + [sds((1, 1), F32)],
        in_specs=[HBM_ANY] * (N_STATE * NMAT) + [in_vmem] * BOTH + [HBM_ANY, in_vmem],
        out_specs=[HBM_ANY] * (NMAT * NMAT) + [pl.BlockSpec(memory_space=pltpu.SMEM)],
        scratch_shapes=[
            pltpu.VMEM((RING_SLOTS, HALF, D), F32),
            pltpu.VMEM((RING_SLOTS, HALF, D), bf16),
            dma((RING_SLOTS,)),
            dma((RING_SLOTS,)),
            dma((RING_SLOTS,)),
            dma((RING_SLOTS,)),
            dma((NMAT * OCT,)),
        ],
        compiler_params=pltpu.CompilerParams(vmem_limit_bytes=SCOPED_BYTES),
        name='write_out',
    )(*late, *held, last_mom, norm_block)


def gelu_fn(values):
    return jax.nn.gelu(values, approximate=True)


def forward(act_in, w_one, w_two, w_three):
    bf16 = jnp.bfloat16
    h_one = jnp.dot(act_in, w_one, preferred_element_type=F32).astype(bf16)
    a_one = gelu_fn(h_one.astype(F32)).astype(bf16)
    y_one = jnp.dot(a_one, w_two, preferred_element_type=F32).astype(bf16)
    h_two = jnp.dot(y_one, w_three, preferred_element_type=F32).astype(bf16)
    a_two = gelu_fn(h_two.astype(F32)).astype(bf16)
    return h_one, a_one, y_one, h_two, a_two


def solution(mesh):
    row_spec = P(('rep', 'data'), None)
    shard_spec = P('data', None)
    full_spec = P()

    def per_device(act_in, grad_out, w_one, w_two, w_three, w_four, master_one, master_two, master_three, master_four, mom_one, mom_two, mom_three, mom_four, vel_one, vel_two, vel_three, vel_four, clip_norm):
        h_one, a_one, y_one, h_two, a_two = forward(act_in, w_one, w_two, w_three)
        acts = (act_in, grad_out, w_two, w_three, w_four, h_one, a_one, y_one, h_two, a_two)
        late, (grads, own_w, last_mom, norm_block) = backward(acts, clip_norm, (master_one, master_two, master_three, master_four), (mom_one, mom_two, mom_three, mom_four), (vel_one, vel_two, vel_three, vel_four))
        *new_state, grad_norm = finish(late, (grads, own_w), last_mom, norm_block)
        return tuple(new_state) + (grad_norm.reshape(()),)

    in_specs = (row_spec, row_spec, full_spec, full_spec, full_spec, full_spec) + (shard_spec,) * 12 + (full_spec,)
    out_specs = (full_spec,) * 4 + (shard_spec,) * 12 + (full_spec,)
    return jax.shard_map(per_device, mesh=mesh, in_specs=in_specs, out_specs=out_specs, check_vma=False)
```
